512 devices in a mesh: member: 2 (over y), seq: 16 (over z), dp: 8 (over x), mp: 2 (over core).
Axes of the slice: x: 8, y: 2, z: 16, core: 2. Of those that a mesh axis runs over, the one named last changes fastest.
The devices are a block of a 8x8x16 slice.
Arguments:
- mixer_in: bfloat16 [16, 2048, 3072], P(('member', 'dp'), 'seq', 'mp'), parts along dimension 0, may hold values from -6 to 6
- delta_raw: bfloat16 [16, 2048, 3072], P(('member', 'dp'), 'seq', 'mp'), parts along dimension 0, may hold values from -2 to 2048
- delta_bias: float32 [6144], P(('member', 'mp')), parts along dimension 0, may hold values from -4 to -2
- decay_log: float32 [6144, 16], P(('member', 'mp')), parts along dimension 0, may hold values from -12 to 1
- skip_gain: float32 [6144], P(('member', 'mp')), parts along dimension 0, may hold values from 0.5 to 1.5
- state_write: bfloat16 [16, 2048, 16], P(('member', 'dp'), 'seq'), parts along dimension 0, may hold values from -5 to 5
- state_read: bfloat16 [16, 2048, 16], P(('member', 'dp'), 'seq'), parts along dimension 0, may hold values from -1.5 to 1.5
- mixer_grad: bfloat16 [16, 2048, 3072], P(('member', 'dp'), 'seq', 'mp'), parts along dimension 0, may hold values from -6 to 6
- attn_query: bfloat16 [16, 2048, 1536], P(('member', 'dp'), 'seq', 'mp'), parts along dimension 0, may hold values from -5 to 5
- attn_key: bfloat16 [16, 2048, 1536], P(('member', 'dp'), 'seq', 'mp'), parts along dimension 0, may hold values from -5 to 5
- attn_value: bfloat16 [16, 2048, 1536], P(('member', 'dp'), 'seq', 'mp'), parts along dimension 0, may hold values from -6 to 6
- attn_grad: bfloat16 [16, 2048, 1536], P(('member', 'dp'), 'seq', 'mp'), parts along dimension 0, may hold values from -6 to 6
- document_id: int32 [16, 2048], P(('member', 'dp'), 'seq'), parts along dimension 0, may hold values from 0 to 3, never falling along the last dimension, each value on 1 to 1024 neighbouring positions
Outputs:
- mixer_out: bfloat16 [16, 2048, 3072], P(('member', 'dp'), 'seq', 'mp'), parts along dimension 0
- input_grad: bfloat16 [16, 2048, 3072], P(('member', 'dp'), 'seq', 'mp'), parts along dimension 0
- delta_grad: bfloat16 [16, 2048, 3072], P(('member', 'dp'), 'seq', 'mp'), parts along dimension 0
- decay_grad: float32 [6144, 16], P(('member', 'mp')), parts along dimension 0
- skip_grad: float32 [6144], P(('member', 'mp')), parts along dimension 0
- bias_grad: float32 [6144], P(('member', 'mp')), parts along dimension 0
- attn_out: bfloat16 [16, 2048, 1536], P(('member', 'dp'), 'seq', 'mp'), parts along dimension 0
- query_grad: bfloat16 [16, 2048, 1536], P(('member', 'dp'), 'seq', 'mp'), parts along dimension 0
- key_grad: bfloat16 [16, 2048, 1536], P(('member', 'dp'), 'seq', 'mp'), parts along dimension 0
- value_grad: bfloat16 [16, 2048, 1536], P(('member', 'dp'), 'seq', 'mp'), parts along dimension 0
The draws below stay inside these ranges and needn't reach their ends.
There are 2 independent parts, one for each index of `member`. The reference program is written for one: setup_inputs(seed, part) draws one part's arguments, and reference() takes and returns one part's arrays. A program takes and returns all parts, laid end to end along the dimension named above; each array names one. Nothing has to cross between parts.
Inputs may be any that keep to these rules, and one draw needn't show every extreme that they name: `document_id`: document numbers never fall along a sequence; a document covers at most 1024 positions.
All inputs are finite; a program needn't handle non-finite values.
Results may differ from the reference program's by a relative error of at most 0.024.
Values may be sent and summed in bfloat16 or wider, within the bound.
A program may use at most 128 MiB of HBM per device.

```python
import math
import jax
import jax.numpy as jnp
import numpy as np
from jax import lax

CH = 3072
STATE = 16
HEADS = 16
HD = 96
DOCS = 4
TOK_DEV = 128
SEQ = 2048
BATCH = 8
WINDOW = 128


def mamba_law(key):
    base = jax.random.fold_in(key, 23)
    parts = jax.random.split(base, 10)
    fast_share = 0.5
    is_fast = jax.random.uniform(parts[0], (CH,)) < fast_share
    fast_rate = jnp.exp(jax.random.uniform(parts[1], (CH,), jnp.float32, math.log(1.0 / 50.0), math.log(1.0 / 30.0)))
    slow_rate = jnp.exp(jax.random.uniform(parts[2], (CH,), jnp.float32, math.log(0.3 / SEQ), math.log(0.9 / SEQ)))
    rate = jnp.where(is_fast, fast_rate, slow_rate)
    base_step = jnp.exp(jax.random.uniform(parts[3], (CH,), jnp.float32, math.log(0.025), math.log(0.1)))
    offset_bias = jnp.log(jnp.expm1(base_step))
    spread = jnp.exp(jax.random.uniform(parts[4], (CH, STATE), jnp.float32, -0.35, 0.35))
    absolute_size = (rate / base_step)[:, None] * spread
    noise = 0.3 * jnp.clip(jax.random.normal(parts[5], (BATCH, SEQ, CH), jnp.float32), -4.0, 4.0)
    regions = jax.random.uniform(parts[6], (BATCH, SEQ // TOK_DEV, 1, CH), jnp.float32, -0.7, 0.7)
    noise = noise + jnp.broadcast_to(regions, (BATCH, SEQ // TOK_DEV, TOK_DEV, CH)).reshape(BATCH, SEQ, CH)
    places = jax.random.randint(parts[7], (BATCH, 3), 0, SEQ)
    objective_value = jax.random.uniform(parts[8], (BATCH, 3), jnp.float32, 0.25, 0.5)
    matched_flag = (places[:, :, None] == jnp.arange(SEQ)[None, None, :]).astype(jnp.float32)
    spike_step_size = (-jnp.log1p(-objective_value))[:, :, None] / jnp.mean(absolute_size, axis=1)[None, None, :]
    spike_raw_values = spike_step_size + jnp.log1p(-jnp.exp(-spike_step_size)) - offset_bias[None, None, :]
    any_hit = jnp.sum(matched_flag, axis=1) > 0.5
    selected_entries = jnp.einsum('ltv,lte->lve', matched_flag, spike_raw_values)
    raw = jnp.where(any_hit[:, :, None], selected_entries, noise)
    write = jnp.clip(jax.random.normal(parts[9], (BATCH, SEQ, STATE), jnp.float32), -5.0, 5.0)
    write = write * jnp.where(any_hit, 0.01, 1.0)[:, :, None]
    return (offset_bias, jnp.log(absolute_size), raw, write)


def attention_law(key):
    base = jax.random.fold_in(key, 41)
    parts = jax.random.split(base, 2)
    width = HEADS * HD
    query = jnp.clip(jax.random.normal(parts[0], (BATCH, SEQ, width), jnp.float32), -5.0, 5.0)
    keyset = jnp.clip(jax.random.normal(parts[1], (BATCH, SEQ, width), jnp.float32), -5.0, 5.0)
    return (query, keyset)


def draw_delta_raw(key, part):
    return mamba_law(key)[2].astype(jnp.bfloat16)


def draw_delta_bias(key, part):
    return mamba_law(key)[0].astype(jnp.float32)


def draw_decay_log(key, part):
    return mamba_law(key)[1].astype(jnp.float32)


def draw_state_write(key, part):
    return mamba_law(key)[3].astype(jnp.bfloat16)


def draw_attn_query(key, part):
    return attention_law(key)[0].astype(jnp.bfloat16)


def draw_attn_key(key, part):
    return attention_law(key)[1].astype(jnp.bfloat16)


def level_of(key, dims, cuts, least, high):
    level = 1.0
    for position, shards_of in cuts:
        heights = jax.random.uniform(jax.random.fold_in(jax.random.fold_in(key, 6), position), (shards_of,), jnp.float32, least / len(cuts), high / len(cuts))
        level = level * jnp.repeat(jnp.exp(heights), dims[position] // shards_of).reshape((-1,) + (1,) * (len(dims) - 1 - position))
    return level


def length_profile(count, total, limit, slope):
    loads = [(1 << 20) // math.isqrt(rank ** slope) + 1 for rank in range(2, count + 1)]
    spare, holding = total - limit - (count - 1), [1] * (count - 1)
    while spare > 0:
        movable = [i for i in range(count - 1) if holding[i] < limit]
        whole, remaining = sum([loads[i] for i in movable]), spare
        for i in movable:
            more = min(limit - holding[i], max(1, remaining * loads[i] // whole), spare)
            holding[i] = holding[i] + more
            spare = spare - more
    return np.array([limit] + holding)


def uneven(rng, amount, total, most, slope):
    if amount == 2:
        one = jax.random.randint(rng, (), max(1, total - most), min(most, total - 1) + 1)
        return jnp.stack([one, total - one])
    tallies = jnp.asarray(length_profile(amount, total, most, slope), jnp.int32)
    pairs = (amount - 1) // 2
    donor, receiver = tallies[1:1 + 2 * pairs:2], tallies[2:2 + 2 * pairs:2]
    margin = jnp.minimum(donor - 1, most - receiver)
    moved = jax.random.randint(jax.random.fold_in(rng, 1), (pairs,), 0, 1 << 20) % (margin + 1)
    tallies = tallies.at[1:1 + 2 * pairs:2].set(donor - moved).at[2:2 + 2 * pairs:2].set(receiver + moved)
    return tallies[jax.random.permutation(jax.random.fold_in(rng, 2), amount)]


def scatter_about(rng, shape, scale, bound, shards=(), dtype=jnp.bfloat16):
    result = jax.random.normal(rng, shape, jnp.float32) * scale
    if len(shards) > 0:
        result = level_of(rng, shape, shards, -0.22, 0.18) * result
    return jnp.clip(result, min=-bound, max=bound).astype(dtype)


def setup_inputs(seed: int = 0, part: int = 0) -> dict:
    key_of = jax.random.split(jax.random.key(seed), 14)
    part_splits = jax.random.split(jax.random.fold_in(key_of[13], part), 14)
    return {
        "mixer_in": scatter_about(part_splits[0], (BATCH, SEQ, CH), 1.0, 6.0, ((0, 8), (1, 16), (2, 2))),
        "delta_raw": draw_delta_raw(jax.random.fold_in(jax.random.fold_in(key_of[13], part), 71), part),
        "delta_bias": draw_delta_bias(jax.random.fold_in(jax.random.fold_in(key_of[13], part), 71), part),
        "decay_log": draw_decay_log(jax.random.fold_in(jax.random.fold_in(key_of[13], part), 71), part),
        "skip_gain": jnp.clip(1.0 + 0.1 * jax.random.normal(part_splits[4], (CH,), jnp.float32), 0.5, 1.5),
        "state_write": draw_state_write(jax.random.fold_in(jax.random.fold_in(key_of[13], part), 71), part),
        "state_read": scatter_about(part_splits[6], (BATCH, SEQ, STATE), 0.25, 1.5, ((0, 8), (1, 16))),
        "mixer_grad": scatter_about(part_splits[7], (BATCH, SEQ, CH), 1.0, 6.0, ((0, 8), (1, 16), (2, 2))),
        "attn_query": draw_attn_query(jax.random.fold_in(jax.random.fold_in(key_of[13], part), 71), part),
        "attn_key": draw_attn_key(jax.random.fold_in(jax.random.fold_in(key_of[13], part), 71), part),
        "attn_value": scatter_about(part_splits[10], (BATCH, SEQ, HEADS * HD), 1.0, 6.0, ((0, 8), (1, 16), (2, 2))),
        "attn_grad": scatter_about(part_splits[11], (BATCH, SEQ, HEADS * HD), 1.0, 6.0, ((0, 8), (1, 16), (2, 2))),
        "document_id": jax.vmap(lambda own: jnp.searchsorted(jnp.cumsum(uneven(own, DOCS, SEQ, SEQ // 2, 0)), jnp.arange(SEQ), side="right"))(jax.random.split(part_splits[12], BATCH)).reshape((BATCH, SEQ)).astype(jnp.int32),
    }


def mamba_group(inputs, raws, grads, writes, reads, decay_log, skip, offset_bias):
    step_size = jax.nn.softplus(raws + offset_bias[None, :])
    rate = -jnp.exp(decay_log)
    weighted = step_size * inputs
    start = jnp.zeros(rate.shape, jnp.float32)

    def advance(state, items):
        sizes, weights, write_row = items
        state = jnp.exp(sizes[:, None] * rate) * state + weights[:, None] * write_row[None, :]
        return (state, state)
    _, states = lax.scan(advance, start, (step_size, weighted, writes))
    mixed = jnp.einsum('ten,tn->te', states, reads, precision=lax.Precision.HIGHEST) + skip[None, :] * inputs
    previous = jnp.concatenate([start[None], states[:-1]], axis=0)

    def retreat(carry, items):
        back, accum = carry
        sizes, values, outs, write_row, read_row, prior = items
        decay = jnp.exp(sizes[:, None] * rate)
        adjoint = read_row[None, :] * outs[:, None] + back
        through_write = lax.optimization_barrier(jnp.sum(adjoint * write_row[None, :], axis=1))
        input_part = through_write * sizes + skip * outs
        tail = adjoint * prior * decay
        step_part = values * through_write + lax.optimization_barrier(jnp.sum(tail * rate, axis=1))
        accum = accum + tail * sizes[:, None]
        return ((decay * adjoint, accum), (input_part, step_part))
    (_, accum), (input_grad, step_grad) = lax.scan(retreat, (start, start), (step_size, inputs, grads, writes, reads, previous), reverse=True)
    raw_grad = step_grad * jax.nn.sigmoid(raws + offset_bias[None, :])
    return (mixed, input_grad, raw_grad, accum * rate, lax.optimization_barrier(jnp.sum(grads * inputs, axis=0)), lax.optimization_barrier(jnp.sum(raw_grad, axis=0)))

def attend_block(items):
    query, key_now, key_before, value_now, value_before, out_grad, doc_now, doc_before = items
    length = query.shape[0]
    width = query.shape[1]
    heads = width // HD
    key_all = jnp.concatenate([key_before, key_now], axis=0).reshape(2 * length, heads, HD).astype(jnp.float32)
    value_all = jnp.concatenate([value_before, value_now], axis=0).reshape(2 * length, heads, HD).astype(jnp.float32)
    doc_all = jnp.concatenate([doc_before, doc_now], axis=0)
    query_heads = query.reshape(length, heads, HD).astype(jnp.float32)
    grad_heads = out_grad.reshape(length, heads, HD).astype(jnp.float32)
    offset = jnp.arange(length)[:, None] + length - jnp.arange(2 * length)[None, :]
    allowed = (offset >= 0) & (offset < WINDOW) & (doc_all[None, :] == doc_now[:, None])
    scale = 1.0 / math.sqrt(HD)
    scores = jnp.einsum('qhd,khd->hqk', query_heads, key_all) * scale
    scores = jnp.where(allowed[None], scores, -1e+30)
    top = lax.optimization_barrier(jnp.max(scores, axis=2))
    total = top + jnp.log(lax.optimization_barrier(jnp.sum(jnp.exp(scores - top[:, :, None]), axis=2)))
    probs = jnp.exp(scores - total[:, :, None])
    probs_low = lax.optimization_barrier(probs.astype(jnp.bfloat16)).astype(jnp.float32)
    attended = jnp.einsum('hqk,khd->qhd', probs_low, value_all).astype(jnp.bfloat16)
    attended_wide = lax.optimization_barrier(attended).astype(jnp.float32)
    row_term = jnp.einsum('qhd,qhd->hq', grad_heads, attended_wide)
    value_score = jnp.einsum('qhd,khd->hqk', grad_heads, value_all)
    score_grad = lax.optimization_barrier((probs * (value_score - row_term[:, :, None])).astype(jnp.bfloat16)).astype(jnp.float32)
    query_grad = (jnp.einsum('hqk,khd->qhd', score_grad, key_all) * scale).astype(jnp.bfloat16)
    key_parts = jnp.einsum('hqk,qhd->khd', score_grad, query_heads) * scale
    value_parts = jnp.einsum('hqk,qhd->khd', probs_low, grad_heads)
    return (attended.reshape(length, width), query_grad.reshape(length, width), key_parts.reshape(2 * length, width), value_parts.reshape(2 * length, width))

def reference(mixer_in, delta_raw, delta_bias, decay_log, skip_gain, state_write, state_read, mixer_grad, attn_query, attn_key, attn_value, attn_grad, document_id):
    group = math.gcd(CH, 512)
    groups = CH // group

    def split_channels(values):
        return values.reshape(SEQ, groups, group).transpose(1, 0, 2)

    def merge_channels(values):
        return values.transpose(1, 0, 2).reshape(SEQ, CH)

    def one_row(items):
        inputs, raws, grads, writes, reads = items
        pieces = (split_channels(inputs), split_channels(raws), split_channels(grads), decay_log.reshape(groups, group, STATE), skip_gain.reshape(groups, group), delta_bias.reshape(groups, group))

        def one_group(piece):
            return mamba_group(piece[0], piece[1], piece[2], writes, reads, piece[3], piece[4], piece[5])
        outs = lax.map(one_group, pieces)
        return (merge_channels(outs[0]).astype(jnp.bfloat16), merge_channels(outs[1]).astype(jnp.bfloat16), merge_channels(outs[2]).astype(jnp.bfloat16), outs[3].reshape(CH, STATE), outs[4].reshape(CH), outs[5].reshape(CH))
    rows = lax.map(one_row, (mixer_in.astype(jnp.float32), delta_raw.astype(jnp.float32), mixer_grad.astype(jnp.float32), state_write.astype(jnp.float32), state_read.astype(jnp.float32)))
    scale = 1.0 / math.sqrt(BATCH * SEQ)
    decay_grad = lax.optimization_barrier(jnp.sum(rows[3], axis=0)) * scale
    skip_grad = lax.optimization_barrier(jnp.sum(rows[4], axis=0)) * scale
    bias_grad = lax.optimization_barrier(jnp.sum(rows[5], axis=0)) * scale
    blocks = SEQ // TOK_DEV
    width = HEADS * HD

    def to_blocks(values):
        return values.reshape(BATCH, blocks, TOK_DEV, width)

    def earlier(values):
        return jnp.concatenate([jnp.zeros_like(values[:, :1]), values[:, :-1]], axis=1)

    def flat(values):
        return values.reshape((BATCH * blocks,) + values.shape[2:])
    query_b = to_blocks(attn_query)
    key_b = to_blocks(attn_key)
    value_b = to_blocks(attn_value)
    grad_b = to_blocks(attn_grad)
    docs = document_id.reshape(BATCH, blocks, TOK_DEV).astype(jnp.int32)
    doc_prev = jnp.concatenate([jnp.full((BATCH, 1, TOK_DEV), -1, jnp.int32), docs[:, :-1]], axis=1)
    outs = lax.map(attend_block, (flat(query_b), flat(key_b), flat(earlier(key_b)), flat(value_b), flat(earlier(value_b)), flat(grad_b), flat(docs), flat(doc_prev)))
    attended = outs[0].reshape(BATCH, SEQ, width)
    query_grad = outs[1].reshape(BATCH, SEQ, width)
    key_parts = outs[2].reshape(BATCH, blocks, 2 * TOK_DEV, width)
    value_parts = outs[3].reshape(BATCH, blocks, 2 * TOK_DEV, width)

    def combine(parts):
        own = parts[:, :, TOK_DEV:]
        before = parts[:, :, :TOK_DEV]
        later = jnp.concatenate([before[:, 1:], jnp.zeros_like(before[:, :1])], axis=1)
        return (own + later).astype(jnp.bfloat16).reshape(BATCH, SEQ, width)
    return (rows[0], rows[1], rows[2], decay_grad, skip_grad, bias_grad, attended, query_grad, combine(key_parts), combine(value_parts))
```

```python
import functools
import math

import jax
import jax.numpy as jnp
from jax import lax
from jax.experimental import pallas as pl
from jax.experimental.pallas import tpu as pltpu
from jax.sharding import PartitionSpec as P

HD = 96
WINDOW = 128
CHUNKS = 8
LANES = 128
BLOCK = 8
NEG = -1e30
BIG = 1e30
LOG2E = math.log2(math.e)
LN2 = math.log(2.0)
MESH = pl.DeviceIdType.MESH
F32 = jnp.float32
BF16 = jnp.bfloat16


def by_distance(count):
    return sorted(range(1, count), key=lambda d: -min(d, count - d))


def exchange(axis, count, me, source, landing, send_sem, recv_sem, slotted):
    copies = []
    for d in by_distance(count):
        peer = lax.rem(me + d, count)
        copy = pltpu.make_async_remote_copy(
            src_ref=source.at[peer] if slotted else source,
            dst_ref=landing.at[me],
            send_sem=send_sem.at[d],
            recv_sem=recv_sem.at[me],
            device_id={axis: peer},
            device_id_type=MESH,
        )
        copy.start()
        copies.append(copy)
    return copies


def arrivals(axis, count, me, source, landing, send_sem, recv_sem, slotted):
    for d in by_distance(count)[::-1]:
        peer = lax.rem(me + d, count)
        pltpu.make_async_remote_copy(
            src_ref=source.at[peer] if slotted else source,
            dst_ref=landing.at[peer],
            send_sem=send_sem.at[d],
            recv_sem=recv_sem.at[peer],
            device_id={axis: peer},
            device_id_type=MESH,
        ).wait_recv()


def shifted_rows(value, steps):
    return pltpu.roll(value, steps % CHUNKS, 0)


def prepare(sizes, x_ref, raw_ref, dy_ref, bias_ref, w_ref, r_ref, sc):
    groups, states, steps = sizes
    for n in range(states):
        sc["wb"][:, n] = jnp.broadcast_to(
            w_ref[:, n : n + 1], (steps * CHUNKS, LANES)
        ).reshape(steps, CHUNKS, LANES)
        sc["rb"][:, n] = jnp.broadcast_to(
            r_ref[:, n : n + 1], (steps * CHUNKS, LANES)
        ).reshape(steps, CHUNKS, LANES)

    def one(g, carry):
        lanes = pl.ds(pl.multiple_of(g * LANES, LANES), LANES)
        z = raw_ref[0, :, lanes].astype(F32) + bias_ref[g]
        small = jnp.exp(-jnp.abs(z))
        step = jnp.maximum(z, 0.0) + jnp.log(1.0 + small)
        sig = jnp.where(z >= 0, 1.0, small) / (1.0 + small)
        for at, value in enumerate(
            (step, sig, x_ref[0, :, lanes].astype(F32), dy_ref[0, :, lanes].astype(F32))
        ):
            sc["nat"][at] = value
            for i in range(steps):
                sc["items"][at, g, i] = sc["nat"].at[at][pl.ds(i, CHUNKS, stride=steps), :]
        return carry

    lax.fori_loop(0, groups, one, 0)


def summarize(sizes, rate_ref, sc):
    groups, states, steps = sizes
    chunk = lax.broadcasted_iota(jnp.int32, (CHUNKS, LANES), 0)

    def one(g, carry):
        total = sc["items"][0, g, 0]
        for i in range(1, steps):
            total = total + sc["items"][0, g, i]
        ahead, behind = ({1: total}, {1: total})
        for d in (1, 2, 4):
            ahead[2 * d] = ahead[d] + jnp.where(chunk >= d, shifted_rows(ahead[d], d), 0.0)
            behind[2 * d] = behind[d] + jnp.where(
                chunk < CHUNKS - d, shifted_rows(behind[d], -d), 0.0
            )
        sc["before"][g] = ahead[8] - total
        sc["after"][g] = behind[8] - total
        whole = ahead[8][CHUNKS - 1 : CHUNKS]
        ahead = {d: jnp.where(chunk >= d, ahead[d], BIG) for d in (1, 2, 4)}
        behind = {d: jnp.where(chunk < CHUNKS - d, behind[d], BIG) for d in (1, 2, 4)}

        for block in range(0, states, BLOCK):
            rate = [
                jnp.broadcast_to(rate_ref[g, n : n + 1, :], (CHUNKS, LANES))
                for n in range(block, block + BLOCK)
            ]

            def lap(i, state):
                ending, leading, through = state
                size = sc["items"][0, g, i]
                weight = size * sc["items"][2, g, i]
                out = sc["items"][3, g, i]
                new_e, new_l, new_t = ([], [], [])
                for k in range(BLOCK):
                    decay = jnp.exp2(rate[k] * size)
                    passed = through[k] * decay
                    new_e.append(decay * ending[k] + weight * sc["wb"][i, block + k])
                    new_l.append(leading[k] + passed * (out * sc["rb"][i, block + k]))
                    new_t.append(passed)
                return (tuple(new_e), tuple(new_l), tuple(new_t))

            zero = jnp.zeros((CHUNKS, LANES), F32)
            ending, leading, _ = lax.fori_loop(
                0,
                steps,
                lap,
                ((zero,) * BLOCK, (zero,) * BLOCK, (jnp.ones((CHUNKS, LANES), F32),) * BLOCK),
                unroll=4,
            )
            for k in range(BLOCK):
                n = block + k
                e, b = (ending[k], leading[k])
                for d in (1, 2, 4):
                    e = e + jnp.exp2(rate[k] * ahead[d]) * shifted_rows(e, d)
                    b = b + jnp.exp2(rate[k] * behind[d]) * shifted_rows(b, -d)
                sc["chunk_e"][g, n] = e
                sc["chunk_b"][g, n] = b
                sc["wide"][n, pl.ds(g, 1), :] = e[CHUNKS - 1 : CHUNKS]
                sc["wide"][n, pl.ds(16 + g, 1), :] = b[0:1]
                sc["wide"][n, pl.ds(32 + g, 1), :] = whole
        return carry

    sc["wide"][...] = jnp.zeros(sc["wide"].shape, F32)
    lax.fori_loop(0, groups, one, 0)
    sc["send1"][...] = sc["wide"][...].astype(BF16)


def starts(count, me, rate_rows_ref, sc):
    sc["recv1"][me] = sc["send1"][me]
    rate = rate_rows_ref[me]
    zero = jnp.zeros((16, LANES), F32)
    state, back = (zero, zero)
    for j in range(count):
        sc["send2"][j, 0:16] = state.astype(BF16)
        ending = sc["recv1"][j, 0:16].astype(F32)
        total = sc["recv1"][j, 32:48].astype(F32)
        state = jnp.exp2(rate * total) * state + ending
        k = count - 1 - j
        sc["send2"][k, 16:32] = back.astype(BF16)
        leading = sc["recv1"][k, 16:32].astype(F32)
        total = sc["recv1"][k, 32:48].astype(F32)
        back = jnp.exp2(rate * total) * back + leading
    sc["recv2"][me] = sc["send2"][me]


def finish(sizes, rate_ref, skip_ref, y_ref, xg_ref, rg_ref, sc):
    groups, states, steps = sizes
    chunk = lax.broadcasted_iota(jnp.int32, (CHUNKS, LANES), 0)
    sc["starts"][...] = sc["recv2"][...].astype(F32)
    sc["sums"][...] = jnp.zeros(sc["sums"].shape, F32)

    def one(g, carry):
        skip = skip_ref[g]
        lanes = pl.ds(pl.multiple_of(g * LANES, LANES), LANES)
        before, after = (sc["before"][g], sc["after"][g])
        for block in range(0, states, BLOCK):
            rate, state, back = ([], [], [])
            for n in range(block, block + BLOCK):
                r = jnp.broadcast_to(rate_ref[g, n : n + 1, :], (CHUNKS, LANES))
                rate.append(r)
                e = jnp.where(chunk >= 1, shifted_rows(sc["chunk_e"][g, n], 1), 0.0)
                b = jnp.where(chunk < CHUNKS - 1, shifted_rows(sc["chunk_b"][g, n], -1), 0.0)
                state.append(e + jnp.exp2(r * before) * sc["starts"][n, pl.ds(g, 1), :])
                back.append(b + jnp.exp2(r * after) * sc["starts"][n, pl.ds(16 + g, 1), :])

            def ahead(i, h):
                size = sc["items"][0, g, i]
                weight = size * sc["items"][2, g, i]
                if block == 0:
                    mixed = skip * sc["items"][2, g, i]
                else:
                    mixed = sc["mixed"][i]
                new = []
                for k in range(BLOCK):
                    moved = jnp.exp2(rate[k] * size) * h[k]
                    sc["moved"][i, k] = moved
                    value = moved + weight * sc["wb"][i, block + k]
                    mixed = mixed + value * sc["rb"][i, block + k]
                    new.append(value)
                sc["mixed"][i] = mixed
                return tuple(new)

            lax.fori_loop(0, steps, ahead, tuple(state), unroll=4)

            def retreat(lap, carry):
                back, total = carry
                i = steps - 1 - lap
                size = sc["items"][0, g, i]
                out = sc["items"][3, g, i]
                if block == 0:
                    written = jnp.zeros((CHUNKS, LANES), F32)
                    turned = jnp.zeros((CHUNKS, LANES), F32)
                else:
                    written = sc["written"][i]
                    turned = sc["turned"][i]
                new_b, new_t = ([], [])
                for k in range(BLOCK):
                    grown = rate[k] * size
                    adjoint = out * sc["rb"][i, block + k] + back[k]
                    written = written + adjoint * sc["wb"][i, block + k]
                    part = adjoint * sc["moved"][i, k] * grown
                    turned = turned + part
                    new_t.append(total[k] + part)
                    new_b.append(jnp.exp2(grown) * adjoint)
                sc["written"][i] = written
                sc["turned"][i] = turned
                return (tuple(new_b), tuple(new_t))

            zero = jnp.zeros((CHUNKS, LANES), F32)
            _, total = lax.fori_loop(
                0, steps, retreat, (tuple(back), (zero,) * BLOCK), unroll=4
            )
            for k in range(BLOCK):
                sc["sums"][block + k, pl.ds(g, 1), :] = LN2 * jnp.sum(
                    total[k], axis=0, keepdims=True
                )
        bias_sum = jnp.zeros((CHUNKS, LANES), F32)
        skip_sum = jnp.zeros((CHUNKS, LANES), F32)
        for i in range(steps):
            size, sig = (sc["items"][0, g, i], sc["items"][1, g, i])
            x, out = (sc["items"][2, g, i], sc["items"][3, g, i])
            written = sc["written"][i]
            raw = (x * written + LN2 * sc["turned"][i] / size) * sig
            bias_sum = bias_sum + raw
            skip_sum = skip_sum + out * x
            rows = pl.ds(i, CHUNKS, stride=steps)
            sc["nat"].at[0][rows, :] = sc["mixed"][i]
            sc["nat"].at[1][rows, :] = written * size + skip * out
            sc["nat"].at[2][rows, :] = raw
        y_ref[0, :, lanes] = sc["nat"][0].astype(BF16)
        xg_ref[0, :, lanes] = sc["nat"][1].astype(BF16)
        rg_ref[0, :, lanes] = sc["nat"][2].astype(BF16)
        sc["sums"][lax.div(g, 2), pl.ds(groups + lax.rem(g, 2), 1), :] = jnp.sum(
            bias_sum, axis=0, keepdims=True
        )
        h = g + groups
        sc["sums"][lax.div(h, 2), pl.ds(groups + lax.rem(h, 2), 1), :] = jnp.sum(
            skip_sum, axis=0, keepdims=True
        )
        return carry

    lax.fori_loop(0, groups, one, 0)
    sc["send3"][...] = sc["sums"][...].astype(BF16)


MIXER_SCRATCH = (
    "wb", "rb", "nat", "items", "before", "after", "chunk_e", "chunk_b", "wide", "send1", "recv1",
    "send2", "recv2", "starts", "sums", "moved", "mixed", "written", "turned", "send3", "recv3",
    "send4", "recv4", "send5", "recv5",
)


def mixer_kernel(sizes, seq, dp, *refs):
    (x_ref, raw_ref, dy_ref, bias_ref, skip_ref, rate_ref, rate_rows_ref, w_ref, r_ref) = refs[:9]
    y_ref, xg_ref, rg_ref, red_ref = refs[9:13]
    sc = dict(zip(MIXER_SCRATCH, refs[13:]))
    send_sem, recv_sem = refs[13 + len(MIXER_SCRATCH) :]
    me = lax.axis_index("seq")
    row = lax.axis_index("dp")

    barrier = pltpu.get_barrier_semaphore()
    for d in range(1, seq):
        pl.semaphore_signal(
            barrier, inc=1, device_id={"seq": lax.rem(me + d, seq)}, device_id_type=MESH
        )
    for d in range(1, dp):
        pl.semaphore_signal(
            barrier, inc=1, device_id={"dp": lax.rem(row + d, dp)}, device_id_type=MESH
        )
    prepare(sizes, x_ref, raw_ref, dy_ref, bias_ref, w_ref, r_ref, sc)
    summarize(sizes, rate_ref, sc)
    pl.semaphore_wait(barrier, seq + dp - 2)

    def run(stage, axis, count, at, source, landing, slotted):
        args = (axis, count, at, source, landing, send_sem.at[stage], recv_sem.at[stage], slotted)
        copies = exchange(*args)
        arrivals(*args)
        return copies

    copies = run(0, "seq", seq, me, sc["send1"], sc["recv1"], True)
    starts(seq, me, rate_rows_ref, sc)
    copies += run(1, "seq", seq, me, sc["send2"], sc["recv2"], True)
    finish(sizes, rate_ref, skip_ref, y_ref, xg_ref, rg_ref, sc)
    copies += run(2, "seq", seq, me, sc["send3"], sc["recv3"], True)
    sc["recv3"][me] = sc["send3"][me]
    part = jnp.sum(sc["recv3"][...].astype(F32), axis=0)
    sc["send4"][...] = part.astype(BF16)
    copies += run(3, "dp", dp, row, sc["send4"], sc["recv4"], False)
    sc["recv4"][row] = sc["send4"][...]
    sc["send5"][...] = jnp.sum(sc["recv4"][...].astype(F32), axis=0).astype(BF16)
    copies += run(4, "seq", seq, me, sc["send5"], sc["recv5"], False)
    sc["recv5"][me] = sc["send5"][...]
    red_ref[...] = sc["recv5"][...].astype(F32)
    for copy in copies:
        copy.wait_send()


def mixer(x, raw, dy, bias, decay_log, skip, write, read):
    seq, dp = (lax.axis_size("seq"), lax.axis_size("dp"))
    _, length, channels = x.shape
    states = decay_log.shape[1]
    groups, steps = (channels // LANES, length // CHUNKS)
    sizes = (groups, states, steps)
    rate = (-LOG2E * jnp.exp(decay_log)).reshape(groups, LANES, states)
    rate_gn = rate.transpose(0, 2, 1)
    rate_ng = jnp.pad(rate.transpose(2, 0, 1), ((0, 0), (0, 16 - groups), (0, 0)))

    def ordered(values):
        return (
            values[0].astype(F32).reshape(CHUNKS, steps, states).transpose(1, 0, 2)
        ).reshape(length, states)

    grid = (steps, states, CHUNKS, LANES)
    line = (steps, CHUNKS, LANES)
    vmem = {
        "wb": (grid, F32),
        "rb": (grid, F32),
        "nat": ((4, length, LANES), F32),
        "items": ((4, groups) + line, F32),
        "before": ((groups, CHUNKS, LANES), F32),
        "after": ((groups, CHUNKS, LANES), F32),
        "chunk_e": ((groups, states, CHUNKS, LANES), F32),
        "chunk_b": ((groups, states, CHUNKS, LANES), F32),
        "wide": ((states, 48, LANES), F32),
        "send1": ((states, 48, LANES), BF16),
        "recv1": ((seq, 48, LANES), BF16),
        "send2": ((seq, 32, LANES), BF16),
        "recv2": ((states, 32, LANES), BF16),
        "starts": ((states, 32, LANES), F32),
        "sums": ((states, 16, LANES), F32),
        "moved": ((steps, BLOCK, CHUNKS, LANES), F32),
        "mixed": (line, F32),
        "written": (line, F32),
        "turned": (line, F32),
        "send3": ((states, 16, LANES), BF16),
        "recv3": ((seq, 16, LANES), BF16),
        "send4": ((16, LANES), BF16),
        "recv4": ((dp, 16, LANES), BF16),
        "send5": ((16, LANES), BF16),
        "recv5": ((states, 16, LANES), BF16),
    }
    inside = pl.BlockSpec(memory_space=pltpu.VMEM)
    y, xg, rg, red = pl.pallas_call(
        functools.partial(mixer_kernel, sizes, seq, dp),
        out_shape=(
            jax.ShapeDtypeStruct(x.shape, BF16),
            jax.ShapeDtypeStruct(x.shape, BF16),
            jax.ShapeDtypeStruct(x.shape, BF16),
            jax.ShapeDtypeStruct((states, 16, LANES), F32),
        ),
        in_specs=[inside] * 9,
        out_specs=(inside,) * 4,
        scratch_shapes=[pltpu.VMEM(*vmem[name]) for name in MIXER_SCRATCH]
        + [pltpu.SemaphoreType.DMA((5, seq))] * 2,
        compiler_params=pltpu.CompilerParams(
            collective_id=0, has_side_effects=True, vmem_limit_bytes=48 << 20
        ),
        cost_estimate=pl.CostEstimate(
            flops=40 * length * channels * states, bytes_accessed=16 * length * channels,
            transcendentals=4 * length * channels * states,
        ),
        name="mixer",
    )(
        x,
        raw,
        dy,
        bias.reshape(groups, 1, LANES),
        skip.reshape(groups, 1, LANES),
        rate_gn,
        rate_ng,
        ordered(write),
        ordered(read),
    )
    scale = 1.0 / math.sqrt(length * seq * dp)
    decay = red[:, :groups].reshape(states, channels).T * scale
    rows = red[:, groups : groups + 2].reshape(2 * states, LANES) * scale
    return (
        y,
        xg,
        rg,
        decay,
        rows[groups : 2 * groups].reshape(channels),
        rows[:groups].reshape(channels),
    )


def window_kernel(
    q_ref, k_ref, v_ref, do_ref, kb_ref, vb_ref, doc_col_ref, doc_row_ref,
    o_ref, dq_ref, dk_ref, dv_ref, dkb_ref, dvb_ref,
):
    length, width = q_ref.shape[1:]
    scale = 1.0 / math.sqrt(HD)
    query = lax.broadcasted_iota(jnp.int32, (length, 2 * length), 0)
    key = lax.broadcasted_iota(jnp.int32, (length, 2 * length), 1)
    offset = query + length - key
    allowed = (offset >= 0) & (offset < WINDOW) & (doc_row_ref[...] == doc_col_ref[...])
    for head in range(width // HD):
        at = slice(head * HD, (head + 1) * HD)
        q, do = (q_ref[0, :, at], do_ref[0, :, at])
        k = jnp.concatenate([kb_ref[0, :, at], k_ref[0, :, at]], axis=0)
        v = jnp.concatenate([vb_ref[0, :, at], v_ref[0, :, at]], axis=0)
        over_lanes = (((1,), (1,)), ((), ()))
        over_rows = (((0,), (0,)), ((), ()))
        plain = (((1,), (0,)), ((), ()))
        scores = lax.dot_general(q, k, over_lanes, preferred_element_type=F32) * scale
        scores = jnp.where(allowed, scores, NEG)
        top = jnp.max(scores, axis=1, keepdims=True)
        raised = jnp.exp(scores - top)
        probs = raised / jnp.sum(raised, axis=1, keepdims=True)
        low = probs.astype(BF16)
        out = lax.dot_general(low, v, plain, preferred_element_type=F32).astype(BF16)
        row_term = jnp.sum(do.astype(F32) * out.astype(F32), axis=1, keepdims=True)
        value_score = lax.dot_general(do, v, over_lanes, preferred_element_type=F32)
        grad = (probs * (value_score - row_term)).astype(BF16)
        o_ref[0, :, at] = out
        dq_ref[0, :, at] = (
            lax.dot_general(grad, k, plain, preferred_element_type=F32) * scale
        ).astype(BF16)
        dk = lax.dot_general(grad, q, over_rows, preferred_element_type=F32) * scale
        dv = lax.dot_general(low, do, over_rows, preferred_element_type=F32)
        dkb_ref[0, :, at] = dk[:length].astype(BF16)
        dvb_ref[0, :, at] = dv[:length].astype(BF16)
        dk_ref[0, :, at] = dk[length:]
        dv_ref[0, :, at] = dv[length:]


def shifted(value, steps):
    count = lax.axis_size("seq")
    leading, last = (max(0, -steps), min(count, count - steps))
    return lax.ppermute(value, "seq", [(source, source + steps) for source in range(leading, last)])


def window(query, key, value, out_grad, docs):
    length = query.shape[1]
    doc_now = docs + 1
    key_before, value_before = (shifted(key, 1), shifted(value, 1))
    doc_before = shifted(doc_now, 1)
    doc_row = jnp.concatenate([doc_before, doc_now], axis=1)
    inside = pl.BlockSpec(memory_space=pltpu.VMEM)
    wide = jax.ShapeDtypeStruct(query.shape, F32)
    low = jax.ShapeDtypeStruct(query.shape, BF16)
    out, dq, dk, dv, dkb, dvb = pl.pallas_call(
        window_kernel,
        out_shape=(low, low, wide, wide, low, low),
        in_specs=[inside] * 8,
        out_specs=(inside,) * 6,
        compiler_params=pltpu.CompilerParams(vmem_limit_bytes=48 << 20),
        cost_estimate=pl.CostEstimate(
            flops=20 * length * length * query.shape[2],
            bytes_accessed=24 * length * query.shape[2],
            transcendentals=0,
        ),
        name="window",
    )(query, key, value, out_grad, key_before, value_before, doc_now.reshape(length, 1), doc_row)
    dk = dk + shifted(dkb, -1).astype(F32)
    dv = dv + shifted(dvb, -1).astype(F32)
    return (out, dq, dk.astype(BF16), dv.astype(BF16))


def body(
    mixer_in,
    delta_raw,
    delta_bias,
    decay_log,
    skip_gain,
    state_write,
    state_read,
    mixer_grad,
    attn_query,
    attn_key,
    attn_value,
    attn_grad,
    document_id,
):
    scanned = mixer(
        mixer_in, delta_raw, mixer_grad, delta_bias, decay_log, skip_gain, state_write, state_read
    )
    attended = window(attn_query, attn_key, attn_value, attn_grad, document_id)
    return scanned + attended


def solution(mesh):
    spread = P(("member", "dp"), "seq", "mp")
    shared = P(("member", "dp"), "seq", None)
    one = P(("member", "mp"))
    two = P(("member", "mp"), None)
    return jax.shard_map(
        body,
        mesh=mesh,
        in_specs=(
            spread,
            spread,
            one,
            two,
            one,
            shared,
            shared,
            spread,
            spread,
            spread,
            spread,
            spread,
            P(("member", "dp"), "seq"),
        ),
        out_specs=(spread, spread, spread, two, one, one, spread, spread, spread, spread),
        check_vma=False,
    )
```

```python
import functools
import math

import jax
import jax.numpy as jnp
from jax import lax
from jax.experimental import pallas as pl
from jax.experimental.pallas import tpu as pltpu
from jax.sharding import PartitionSpec as P

HD = 96
WINDOW = 128
CHUNKS = 8
LANES = 128
BLOCK = 8
NEG = -1e30
BIG = 1e30
LOG2E = math.log2(math.e)
LN2 = math.log(2.0)
MESH = pl.DeviceIdType.MESH
F32 = jnp.float32
BF16 = jnp.bfloat16


def by_distance(count):
    return sorted(range(1, count), key=lambda d: -min(d, count - d))


def exchange(axis, count, me, source, landing, send_sem, recv_sem, slotted):
    copies = []
    for d in by_distance(count):
        peer = lax.rem(me + d, count)
        copy = pltpu.make_async_remote_copy(
            src_ref=source.at[peer] if slotted else source,
            dst_ref=landing.at[me],
            send_sem=send_sem.at[d],
            recv_sem=recv_sem.at[me],
            device_id={axis: peer},
            device_id_type=MESH,
        )
        copy.start()
        copies.append(copy)
    return copies


def arrivals(axis, count, me, source, landing, send_sem, recv_sem, slotted):
    for d in by_distance(count)[::-1]:
        peer = lax.rem(me + d, count)
        pltpu.make_async_remote_copy(
            src_ref=source.at[peer] if slotted else source,
            dst_ref=landing.at[peer],
            send_sem=send_sem.at[d],
            recv_sem=recv_sem.at[peer],
            device_id={axis: peer},
            device_id_type=MESH,
        ).wait_recv()


def shifted_rows(value, steps):
    return pltpu.roll(value, steps % CHUNKS, 0)


def prepare(sizes, me, bias_ref, decay_ref, write_ref, read_ref, sc):
    groups, states, steps = sizes
    rate = -LOG2E * jnp.exp(decay_ref[...])
    for g in range(groups):
        sc["rate"][g] = rate[:, g * LANES : (g + 1) * LANES]
    sc["mine"][...] = jnp.zeros(sc["mine"].shape, F32)
    for g in range(groups):
        sc["mine"][g : g + 1] = sc["rate"][g, pl.ds(me, 1), :]
    for source, name in ((write_ref, "wb"), (read_ref, "rb")):
        sc["nat"][0, :, 0:states] = source[0].astype(F32).T
        for i in range(steps):
            rows = sc["nat"].at[0][pl.ds(i, CHUNKS, stride=steps), :]
            for n in range(states):
                sc[name][i, n] = jnp.broadcast_to(rows[:, n : n + 1], (CHUNKS, LANES))

    def one(g, carry):
        lanes = pl.ds(pl.multiple_of(g * LANES, LANES), LANES)
        z = sc["raw"][:, lanes].astype(F32) + bias_ref[:, lanes]
        small = jnp.exp(-jnp.abs(z))
        step = jnp.maximum(z, 0.0) + jnp.log(1.0 + small)
        sig = jnp.where(z >= 0, 1.0, small) / (1.0 + small)
        for at, value in enumerate(
            (step, sig, sc["x"][:, lanes].astype(F32), sc["dy"][:, lanes].astype(F32))
        ):
            sc["nat"][at] = value
            for i in range(steps):
                sc["items"][at, g, i] = sc["nat"].at[at][pl.ds(i, CHUNKS, stride=steps), :]
        return carry

    lax.fori_loop(0, groups, one, 0)


def summarize(sizes, sc):
    groups, states, steps = sizes
    chunk = lax.broadcasted_iota(jnp.int32, (CHUNKS, LANES), 0)

    def one(g, carry):
        total = sc["items"][0, g, 0]
        for i in range(1, steps):
            total = total + sc["items"][0, g, i]
        ahead, behind = ({1: total}, {1: total})
        for d in (1, 2, 4):
            ahead[2 * d] = ahead[d] + jnp.where(chunk >= d, shifted_rows(ahead[d], d), 0.0)
            behind[2 * d] = behind[d] + jnp.where(
                chunk < CHUNKS - d, shifted_rows(behind[d], -d), 0.0
            )
        sc["before"][g] = ahead[8] - total
        sc["after"][g] = behind[8] - total
        whole = ahead[8][CHUNKS - 1 : CHUNKS]
        ahead = {d: jnp.where(chunk >= d, ahead[d], BIG) for d in (1, 2, 4)}
        behind = {d: jnp.where(chunk < CHUNKS - d, behind[d], BIG) for d in (1, 2, 4)}

        for block in range(0, states, BLOCK):
            rate = [
                jnp.broadcast_to(sc["rate"][g, n : n + 1, :], (CHUNKS, LANES))
                for n in range(block, block + BLOCK)
            ]

            def lap(i, state):
                ending, leading, through = state
                size = sc["items"][0, g, i]
                weight = size * sc["items"][2, g, i]
                out = sc["items"][3, g, i]
                new_e, new_l, new_t = ([], [], [])
                for k in range(BLOCK):
                    decay = jnp.exp2(rate[k] * size)
                    passed = through[k] * decay
                    new_e.append(decay * ending[k] + weight * sc["wb"][i, block + k])
                    new_l.append(leading[k] + passed * (out * sc["rb"][i, block + k]))
                    new_t.append(passed)
                return (tuple(new_e), tuple(new_l), tuple(new_t))

            zero = jnp.zeros((CHUNKS, LANES), F32)
            ending, leading, _ = lax.fori_loop(
                0,
                steps,
                lap,
                ((zero,) * BLOCK, (zero,) * BLOCK, (jnp.ones((CHUNKS, LANES), F32),) * BLOCK),
                unroll=4,
            )
            for k in range(BLOCK):
                n = block + k
                e, b = (ending[k], leading[k])
                for d in (1, 2, 4):
                    e = e + jnp.exp2(rate[k] * ahead[d]) * shifted_rows(e, d)
                    b = b + jnp.exp2(rate[k] * behind[d]) * shifted_rows(b, -d)
                sc["chunk_e"][g, n] = e
                sc["chunk_b"][g, n] = b
                sc["wide"][n, pl.ds(g, 1), :] = e[CHUNKS - 1 : CHUNKS]
                sc["wide"][n, pl.ds(16 + g, 1), :] = b[0:1]
                sc["wide"][n, pl.ds(32 + g, 1), :] = whole
        return carry

    sc["wide"][...] = jnp.zeros(sc["wide"].shape, F32)
    lax.fori_loop(0, groups, one, 0)
    sc["send1"][...] = sc["wide"][...].astype(BF16)


def starts(count, me, sc):
    sc["recv1"][me] = sc["send1"][me]
    rate = sc["mine"][...]
    zero = jnp.zeros((16, LANES), F32)
    state, back = (zero, zero)
    for j in range(count):
        sc["send2"][j, 0:16] = state.astype(BF16)
        ending = sc["recv1"][j, 0:16].astype(F32)
        total = sc["recv1"][j, 32:48].astype(F32)
        state = jnp.exp2(rate * total) * state + ending
        k = count - 1 - j
        sc["send2"][k, 16:32] = back.astype(BF16)
        leading = sc["recv1"][k, 16:32].astype(F32)
        total = sc["recv1"][k, 32:48].astype(F32)
        back = jnp.exp2(rate * total) * back + leading
    sc["recv2"][me] = sc["send2"][me]


def finish(sizes, skip_ref, y_ref, xg_ref, rg_ref, sc):
    groups, states, steps = sizes
    chunk = lax.broadcasted_iota(jnp.int32, (CHUNKS, LANES), 0)
    sc["starts"][...] = sc["recv2"][...].astype(F32)
    sc["sums"][...] = jnp.zeros(sc["sums"].shape, F32)

    def one(g, carry):
        lanes = pl.ds(pl.multiple_of(g * LANES, LANES), LANES)
        skip = skip_ref[:, lanes]
        before, after = (sc["before"][g], sc["after"][g])
        for block in range(0, states, BLOCK):
            rate, state, back = ([], [], [])
            for n in range(block, block + BLOCK):
                r = jnp.broadcast_to(sc["rate"][g, n : n + 1, :], (CHUNKS, LANES))
                rate.append(r)
                e = jnp.where(chunk >= 1, shifted_rows(sc["chunk_e"][g, n], 1), 0.0)
                b = jnp.where(chunk < CHUNKS - 1, shifted_rows(sc["chunk_b"][g, n], -1), 0.0)
                state.append(e + jnp.exp2(r * before) * sc["starts"][n, pl.ds(g, 1), :])
                back.append(b + jnp.exp2(r * after) * sc["starts"][n, pl.ds(16 + g, 1), :])

            def ahead(i, h):
                size = sc["items"][0, g, i]
                weight = size * sc["items"][2, g, i]
                if block == 0:
                    mixed = skip * sc["items"][2, g, i]
                else:
                    mixed = sc["mixed"][i]
                new = []
                for k in range(BLOCK):
                    moved = jnp.exp2(rate[k] * size) * h[k]
                    sc["moved"][i, k] = moved
                    value = moved + weight * sc["wb"][i, block + k]
                    mixed = mixed + value * sc["rb"][i, block + k]
                    new.append(value)
                sc["mixed"][i] = mixed
                return tuple(new)

            lax.fori_loop(0, steps, ahead, tuple(state), unroll=4)

            def retreat(lap, carry):
                back, total = carry
                i = steps - 1 - lap
                size = sc["items"][0, g, i]
                out = sc["items"][3, g, i]
                if block == 0:
                    written = jnp.zeros((CHUNKS, LANES), F32)
                    turned = jnp.zeros((CHUNKS, LANES), F32)
                else:
                    written = sc["written"][i]
                    turned = sc["turned"][i]
                new_b, new_t = ([], [])
                for k in range(BLOCK):
                    grown = rate[k] * size
                    adjoint = out * sc["rb"][i, block + k] + back[k]
                    written = written + adjoint * sc["wb"][i, block + k]
                    part = adjoint * sc["moved"][i, k] * grown
                    turned = turned + part
                    new_t.append(total[k] + part)
                    new_b.append(jnp.exp2(grown) * adjoint)
                sc["written"][i] = written
                sc["turned"][i] = turned
                return (tuple(new_b), tuple(new_t))

            zero = jnp.zeros((CHUNKS, LANES), F32)
            _, total = lax.fori_loop(
                0, steps, retreat, (tuple(back), (zero,) * BLOCK), unroll=4
            )
            for k in range(BLOCK):
                sc["sums"][block + k, pl.ds(g, 1), :] = LN2 * jnp.sum(
                    total[k], axis=0, keepdims=True
                )
        bias_sum = jnp.zeros((CHUNKS, LANES), F32)
        skip_sum = jnp.zeros((CHUNKS, LANES), F32)
        for i in range(steps):
            size, sig = (sc["items"][0, g, i], sc["items"][1, g, i])
            x, out = (sc["items"][2, g, i], sc["items"][3, g, i])
            written = sc["written"][i]
            raw = (x * written + LN2 * sc["turned"][i] / size) * sig
            bias_sum = bias_sum + raw
            skip_sum = skip_sum + out * x
            rows = pl.ds(i, CHUNKS, stride=steps)
            sc["nat"].at[0][rows, :] = sc["mixed"][i]
            sc["nat"].at[1][rows, :] = written * size + skip * out
            sc["nat"].at[2][rows, :] = raw
        y_ref[0, :, lanes] = sc["nat"][0].astype(BF16)
        xg_ref[0, :, lanes] = sc["nat"][1].astype(BF16)
        rg_ref[0, :, lanes] = sc["nat"][2].astype(BF16)
        sc["sums"][lax.div(g, 2), pl.ds(groups + lax.rem(g, 2), 1), :] = jnp.sum(
            bias_sum, axis=0, keepdims=True
        )
        h = g + groups
        sc["sums"][lax.div(h, 2), pl.ds(groups + lax.rem(h, 2), 1), :] = jnp.sum(
            skip_sum, axis=0, keepdims=True
        )
        return carry

    lax.fori_loop(0, groups, one, 0)
    sc["send3"][...] = sc["sums"][...].astype(BF16)


def window(first, o_ref, dq_ref, doc_ref, sc):
    length, width = sc["q"].shape
    scale = 1.0 / math.sqrt(HD)
    docs = doc_ref[...]
    before = jnp.where(first, -1, sc["doc_in"][...])
    own = jnp.broadcast_to(docs.astype(F32), (length, length)).T
    own = jnp.concatenate([own, own], axis=1)
    seen = jnp.concatenate([before, docs], axis=1).astype(F32)
    query = lax.broadcasted_iota(jnp.int32, (length, 2 * length), 0)
    key = lax.broadcasted_iota(jnp.int32, (length, 2 * length), 1)
    offset = query + length - key
    allowed = (offset >= 0) & (offset < WINDOW) & (own == seen)
    over_lanes = (((1,), (1,)), ((), ()))
    over_rows = (((0,), (0,)), ((), ()))
    plain = (((1,), (0,)), ((), ()))
    for head in range(width // HD):
        at = slice(head * HD, (head + 1) * HD)
        q, do = (sc["q"][:, at], sc["do"][:, at])
        k = jnp.concatenate([sc["k_in"][:, at], sc["k"][:, at]], axis=0)
        v = jnp.concatenate([sc["v_in"][:, at], sc["v"][:, at]], axis=0)
        scores = lax.dot_general(q, k, over_lanes, preferred_element_type=F32) * scale
        scores = jnp.where(allowed, scores, NEG)
        top = jnp.max(scores, axis=1, keepdims=True)
        raised = jnp.exp(scores - top)
        probs = raised / jnp.sum(raised, axis=1, keepdims=True)
        low = probs.astype(BF16)
        out = lax.dot_general(low, v, plain, preferred_element_type=F32).astype(BF16)
        row_term = jnp.sum(do.astype(F32) * out.astype(F32), axis=1, keepdims=True)
        value_score = lax.dot_general(do, v, over_lanes, preferred_element_type=F32)
        grad = (probs * (value_score - row_term)).astype(BF16)
        o_ref[0, :, at] = out
        dq_ref[0, :, at] = (
            lax.dot_general(grad, k, plain, preferred_element_type=F32) * scale
        ).astype(BF16)
        dk = lax.dot_general(grad, q, over_rows, preferred_element_type=F32) * scale
        dv = lax.dot_general(low, do, over_rows, preferred_element_type=F32)
        sc["dk_out"][:, at] = dk[:length].astype(BF16)
        sc["dv_out"][:, at] = dv[:length].astype(BF16)
        sc["dk"][:, at] = dk[length:]
        sc["dv"][:, at] = dv[length:]


SEMAPHORES = ("load", "send", "recv", "halo_send", "halo_recv")


def scratch_shapes(sizes, length, width, seq, dp):
    groups, states, steps = sizes
    channels = groups * LANES
    grid = (steps, states, CHUNKS, LANES)
    line = (steps, CHUNKS, LANES)
    return {
        "x": ((length, channels), BF16),
        "raw": ((length, channels), BF16),
        "dy": ((length, channels), BF16),
        "q": ((length, width), BF16),
        "k": ((length, width), BF16),
        "v": ((length, width), BF16),
        "do": ((length, width), BF16),
        "k_in": ((length, width), BF16),
        "v_in": ((length, width), BF16),
        "doc_in": ((1, length), jnp.int32),
        "dk": ((length, width), F32),
        "dv": ((length, width), F32),
        "dk_out": ((length, width), BF16),
        "dv_out": ((length, width), BF16),
        "dk_in": ((length, width), BF16),
        "dv_in": ((length, width), BF16),
        "rate": ((groups, states, LANES), F32),
        "mine": ((16, LANES), F32),
        "wb": (grid, F32),
        "rb": (grid, F32),
        "nat": ((4, length, LANES), F32),
        "items": ((4, groups) + line, F32),
        "before": ((groups, CHUNKS, LANES), F32),
        "after": ((groups, CHUNKS, LANES), F32),
        "chunk_e": ((groups, states, CHUNKS, LANES), F32),
        "chunk_b": ((groups, states, CHUNKS, LANES), F32),
        "wide": ((states, 48, LANES), F32),
        "send1": ((states, 48, LANES), BF16),
        "recv1": ((seq, 48, LANES), BF16),
        "send2": ((seq, 32, LANES), BF16),
        "recv2": ((states, 32, LANES), BF16),
        "starts": ((states, 32, LANES), F32),
        "sums": ((states, 16, LANES), F32),
        "moved": ((steps, BLOCK, CHUNKS, LANES), F32),
        "mixed": (line, F32),
        "written": (line, F32),
        "turned": (line, F32),
        "send3": ((states, 16, LANES), BF16),
        "recv3": ((seq, 16, LANES), BF16),
        "send4": ((16, LANES), BF16),
        "recv4": ((dp, 16, LANES), BF16),
        "send5": ((16, LANES), BF16),
        "recv5": ((states, 16, LANES), BF16),
    }


def step_kernel(sizes, seq, dp, names, *refs):
    groups, states, steps = sizes
    hbm, (bias_ref, skip_ref, decay_ref, write_ref, read_ref, doc_ref) = (refs[:7], refs[7:13])
    y_ref, xg_ref, rg_ref, o_ref, dq_ref, dk_ref, dv_ref = refs[13:20]
    decay_out, skip_out, bias_out = refs[20:23]
    sc = dict(zip(names, refs[23:]))
    load_sem, send_sem, recv_sem, halo_send, halo_recv = refs[23 + len(names) :]
    me = lax.axis_index("seq")
    row = lax.axis_index("dp")

    loads = [
        pltpu.make_async_copy(source.at[0], sc[name], load_sem.at[at])
        for at, (source, name) in enumerate(zip(hbm, ("x", "raw", "dy", "q", "k", "v", "do")))
    ]
    for load in loads:
        load.start()
    barrier = pltpu.get_barrier_semaphore()
    for d in range(1, seq):
        pl.semaphore_signal(
            barrier, inc=1, device_id={"seq": lax.rem(me + d, seq)}, device_id_type=MESH
        )
    for d in range(1, dp):
        pl.semaphore_signal(
            barrier, inc=1, device_id={"dp": lax.rem(row + d, dp)}, device_id_type=MESH
        )
    for load in loads[:3]:
        load.wait()
    prepare(sizes, me, bias_ref, decay_ref, write_ref, read_ref, sc)
    summarize(sizes, sc)
    for load in loads[3:]:
        load.wait()
    pl.semaphore_wait(barrier, seq + dp - 2)

    def args(stage, axis, count, at, source, landing, slotted):
        return (
            axis, count, at, sc[source], sc[landing], send_sem.at[stage], recv_sem.at[stage], slotted
        )

    def halo(at, source, landing, steps):
        return pltpu.make_async_remote_copy(
            src_ref=source,
            dst_ref=sc[landing],
            send_sem=halo_send.at[at],
            recv_sem=halo_recv.at[at],
            device_id={"seq": lax.rem(me + steps + seq, seq)},
            device_id_type=MESH,
        )

    stage = args(0, "seq", seq, me, "send1", "recv1", True)
    copies = exchange(*stage)
    ahead = [
        halo(0, sc["k"], "k_in", 1),
        halo(1, sc["v"], "v_in", 1),
        halo(2, doc_ref, "doc_in", 1),
    ]
    for copy in ahead:
        copy.start()
    arrivals(*stage)
    starts(seq, me, sc)
    stage = args(1, "seq", seq, me, "send2", "recv2", True)
    copies += exchange(*stage)
    for copy in ahead:
        copy.wait_recv()
    window(me == 0, o_ref, dq_ref, doc_ref, sc)
    behind = [halo(3, sc["dk_out"], "dk_in", -1), halo(4, sc["dv_out"], "dv_in", -1)]
    for copy in behind:
        copy.start()
    arrivals(*stage)
    finish(sizes, skip_ref, y_ref, xg_ref, rg_ref, sc)
    stage = args(2, "seq", seq, me, "send3", "recv3", True)
    copies += exchange(*stage)
    for copy in behind:
        copy.wait_recv()
    dk_ref[0] = (sc["dk"][...] + sc["dk_in"][...].astype(F32)).astype(BF16)
    dv_ref[0] = (sc["dv"][...] + sc["dv_in"][...].astype(F32)).astype(BF16)
    arrivals(*stage)
    sc["recv3"][me] = sc["send3"][me]
    sc["send4"][...] = jnp.sum(sc["recv3"][...].astype(F32), axis=0).astype(BF16)
    stage = args(3, "dp", dp, row, "send4", "recv4", False)
    copies += exchange(*stage)
    arrivals(*stage)
    sc["recv4"][row] = sc["send4"][...]
    sc["send5"][...] = jnp.sum(sc["recv4"][...].astype(F32), axis=0).astype(BF16)
    stage = args(4, "seq", seq, me, "send5", "recv5", False)
    copies += exchange(*stage)
    arrivals(*stage)
    sc["recv5"][me] = sc["send5"][...]
    scale = 1.0 / math.sqrt(steps * CHUNKS * seq * dp)
    sc["sums"][...] = sc["recv5"][...].astype(F32) * scale
    for g in range(groups):
        lanes = slice(g * LANES, (g + 1) * LANES)
        decay_out[:, lanes] = sc["sums"][:, g, :]
        bias_out[:, lanes] = sc["sums"][g // 2, groups + g % 2 : groups + g % 2 + 1, :]
        h = g + groups
        skip_out[:, lanes] = sc["sums"][h // 2, groups + h % 2 : groups + h % 2 + 1, :]
    for copy in copies + ahead + behind:
        copy.wait_send()


def flush_kernel(*refs):
    count = len(refs) // 2
    sem = refs[-1]
    copies = [
        pltpu.make_async_copy(refs[at], refs[count + at], sem.at[at]) for at in range(count)
    ]
    for copy in copies:
        copy.start()
    for copy in copies:
        copy.wait()


def body(
    mixer_in,
    delta_raw,
    delta_bias,
    decay_log,
    skip_gain,
    state_write,
    state_read,
    mixer_grad,
    attn_query,
    attn_key,
    attn_value,
    attn_grad,
    document_id,
):
    seq, dp = (lax.axis_size("seq"), lax.axis_size("dp"))
    _, length, channels = mixer_in.shape
    width = attn_query.shape[2]
    states = decay_log.shape[1]
    sizes = (channels // LANES, states, length // CHUNKS)
    scratch = scratch_shapes(sizes, length, width, seq, dp)
    inside = pl.BlockSpec(memory_space=pltpu.VMEM)
    outside = pl.BlockSpec(memory_space=pltpu.HBM)
    shapes = (
        [jax.ShapeDtypeStruct(mixer_in.shape, BF16)] * 3
        + [jax.ShapeDtypeStruct(attn_query.shape, BF16)] * 4
        + [jax.ShapeDtypeStruct((states, channels), F32)]
        + [jax.ShapeDtypeStruct((1, channels), F32)] * 2
    )
    results = pl.pallas_call(
        functools.partial(step_kernel, sizes, seq, dp, tuple(scratch)),
        out_shape=tuple(shapes),
        in_specs=[outside] * 7 + [inside] * 6,
        out_specs=(inside,) * len(shapes),
        scratch_shapes=[pltpu.VMEM(*shape) for shape in scratch.values()]
        + [
            pltpu.SemaphoreType.DMA((7,)),
            pltpu.SemaphoreType.DMA((5, seq)),
            pltpu.SemaphoreType.DMA((5, seq)),
            pltpu.SemaphoreType.DMA((5,)),
            pltpu.SemaphoreType.DMA((5,)),
        ],
        compiler_params=pltpu.CompilerParams(
            collective_id=0, has_side_effects=True, vmem_limit_bytes=48 << 20
        ),
        name="step",
    )(
        pltpu.with_memory_space_constraint(mixer_in, pltpu.HBM),
        pltpu.with_memory_space_constraint(delta_raw, pltpu.HBM),
        pltpu.with_memory_space_constraint(mixer_grad, pltpu.HBM),
        pltpu.with_memory_space_constraint(attn_query, pltpu.HBM),
        pltpu.with_memory_space_constraint(attn_key, pltpu.HBM),
        pltpu.with_memory_space_constraint(attn_value, pltpu.HBM),
        pltpu.with_memory_space_constraint(attn_grad, pltpu.HBM),
        delta_bias.reshape(1, channels),
        skip_gain.reshape(1, channels),
        decay_log.T,
        state_write.transpose(0, 2, 1),
        state_read.transpose(0, 2, 1),
        document_id,
    )
    results = pl.pallas_call(
        flush_kernel,
        out_shape=tuple(shapes),
        in_specs=[inside] * len(shapes),
        out_specs=(outside,) * len(shapes),
        scratch_shapes=[pltpu.SemaphoreType.DMA((len(shapes),))],
        compiler_params=pltpu.CompilerParams(vmem_limit_bytes=1 << 20),
        name="flush",
    )(*results)
    y, xg, rg, o, dq, dk, dv, decay, skip, bias = results
    return (y, xg, rg, decay.T, skip.reshape(channels), bias.reshape(channels), o, dq, dk, dv)


def solution(mesh):
    spread = P(("member", "dp"), "seq", "mp")
    shared = P(("member", "dp"), "seq", None)
    one = P(("member", "mp"))
    two = P(("member", "mp"), None)
    return jax.shard_map(
        body,
        mesh=mesh,
        in_specs=(
            spread,
            spread,
            one,
            two,
            one,
            shared,
            shared,
            spread,
            spread,
            spread,
            spread,
            spread,
            P(("member", "dp"), "seq"),
        ),
        out_specs=(spread, spread, spread, two, one, one, spread, spread, spread, spread),
        check_vma=False,
    )
```

```python
import functools
import math
import types

import jax
import jax.numpy as jnp
from jax import lax
from jax.experimental import pallas as pl
from jax.experimental.pallas import tpu as pltpu
from jax.sharding import PartitionSpec as P

HD = 96
WINDOW = 128
CHUNKS = 8
LANES = 128
BLOCK = 8
SMALL = 4
NEG = -1e30
BIG = 1e30
LOG2E = math.log2(math.e)
LN2 = math.log(2.0)
MESH = pl.DeviceIdType.MESH
F32 = jnp.float32
BF16 = jnp.bfloat16


def by_distance(count):
    return sorted(range(1, count), key=lambda d: -min(d, count - d))


def exchange(axis, count, me, source, landing, send_sem, recv_sem, slotted):
    copies = []
    for d in by_distance(count):
        peer = lax.rem(me + d, count)
        copy = pltpu.make_async_remote_copy(
            src_ref=source.at[peer] if slotted else source,
            dst_ref=landing.at[me],
            send_sem=send_sem.at[d],
            recv_sem=recv_sem.at[me],
            device_id={axis: peer},
            device_id_type=MESH,
        )
        copy.start()
        copies.append(copy)
    return copies


def arrivals(axis, count, me, source, landing, send_sem, recv_sem, slotted, origins):
    for j in origins:

        @pl.when(me != j)
        def _():
            pltpu.make_async_remote_copy(
                src_ref=source.at[j] if slotted else source,
                dst_ref=landing.at[j],
                send_sem=send_sem.at[0],
                recv_sem=recv_sem.at[j],
                device_id={axis: j},
                device_id_type=MESH,
            ).wait_recv()


def tree(terms):
    while len(terms) > 1:
        terms = [
            terms[at] + terms[at + 1] if at + 1 < len(terms) else terms[at]
            for at in range(0, len(terms), 2)
        ]
    return terms[0]


def shifted_rows(value, steps):
    return pltpu.roll(value, steps % CHUNKS, 0)


def prepare(sizes, arrived, sc):
    groups, states, steps = sizes
    rate = -LOG2E * jnp.exp(sc.decay[...])
    sc.lined[...] = jnp.zeros(sc.lined.shape, F32)
    for g in range(groups):
        sc.rate[g] = rate[:, g * LANES : (g + 1) * LANES]
        sc.lined[:, g] = rate[:, g * LANES : (g + 1) * LANES]
    for ref in (sc.coef, sc.rows):
        ref[...] = jnp.zeros(ref.shape, F32)
    for source, wide in ((sc.write, sc.wb), (sc.read, sc.rb)):
        sc.nat[0, :, 0:states] = source[0].astype(F32).T
        for i in range(steps):
            rows = sc.nat.at[0][pl.ds(i, CHUNKS, stride=steps), :]
            for n in range(states):
                wide[i, n] = jnp.broadcast_to(rows[:, n : n + 1], (CHUNKS, LANES))
    arrived()

    def one(g, carry):
        lanes = pl.ds(pl.multiple_of(g * LANES, LANES), LANES)
        z = sc.raw[:, lanes].astype(F32) + sc.bias[:, lanes]
        small = jnp.exp(-jnp.abs(z))
        step = jnp.maximum(z, 0.0) + jnp.log(1.0 + small)
        sig = jnp.where(z >= 0, 1.0, small) / (1.0 + small)
        for at, value in enumerate(
            (step, sig, sc.x[:, lanes].astype(F32), sc.dy[:, lanes].astype(F32))
        ):
            sc.nat[at] = value
            for i in range(steps):
                sc.items[at, g, i] = sc.nat.at[at][pl.ds(i, CHUNKS, stride=steps), :]
        return carry

    lax.fori_loop(0, groups, one, 0)


def summarize(sizes, sc):
    groups, states, steps = sizes
    chunk = lax.broadcasted_iota(jnp.int32, (CHUNKS, LANES), 0)

    def one(g, carry):
        total = sc.items[0, g, 0]
        for i in range(1, steps):
            total = total + sc.items[0, g, i]
        ahead, behind = ({1: total}, {1: total})
        for d in (1, 2, 4):
            ahead[2 * d] = ahead[d] + jnp.where(chunk >= d, shifted_rows(ahead[d], d), 0.0)
            behind[2 * d] = behind[d] + jnp.where(
                chunk < CHUNKS - d, shifted_rows(behind[d], -d), 0.0
            )
        sc.before[g] = ahead[8] - total
        sc.after[g] = behind[8] - total
        whole = ahead[8][CHUNKS - 1 : CHUNKS]
        ahead = {d: jnp.where(chunk >= d, ahead[d], BIG) for d in (1, 2, 4)}
        behind = {d: jnp.where(chunk < CHUNKS - d, behind[d], BIG) for d in (1, 2, 4)}

        for block in range(0, states, BLOCK):
            rate = [
                jnp.broadcast_to(sc.rate[g, n : n + 1, :], (CHUNKS, LANES))
                for n in range(block, block + BLOCK)
            ]

            def lap(i, state):
                ending, leading, through = state
                size = sc.items[0, g, i]
                weight = size * sc.items[2, g, i]
                out = sc.items[3, g, i]
                new_e, new_l, new_t = ([], [], [])
                for k in range(BLOCK):
                    decay = jnp.exp2(rate[k] * size)
                    passed = through[k] * decay
                    new_e.append(decay * ending[k] + weight * sc.wb[i, block + k])
                    new_l.append(leading[k] + passed * (out * sc.rb[i, block + k]))
                    new_t.append(passed)
                return (tuple(new_e), tuple(new_l), tuple(new_t))

            zero = jnp.zeros((CHUNKS, LANES), F32)
            ending, leading, _ = lax.fori_loop(
                0,
                steps,
                lap,
                ((zero,) * BLOCK, (zero,) * BLOCK, (jnp.ones((CHUNKS, LANES), F32),) * BLOCK),
                unroll=16,
            )
            for k in range(BLOCK):
                n = block + k
                e, b = (ending[k], leading[k])
                for d in (1, 2, 4):
                    e = e + jnp.exp2(rate[k] * ahead[d]) * shifted_rows(e, d)
                    b = b + jnp.exp2(rate[k] * behind[d]) * shifted_rows(b, -d)
                sc.chunk_e[g, n] = e
                sc.chunk_b[g, n] = b
                sc.wide[n, pl.ds(g, 1), :] = e[CHUNKS - 1 : CHUNKS]
                sc.wide[n, pl.ds(16 + g, 1), :] = b[0:1]
                sc.wide[n, pl.ds(32 + g, 1), :] = whole
        return carry

    sc.wide[...] = jnp.zeros(sc.wide.shape, F32)
    lax.fori_loop(0, groups, one, 0)
    sc.send1[...] = sc.wide[...].astype(BF16)


def forward_starts(count, me, sc):
    sc.recv1[me] = sc.send1[me]
    rate = sc.lined[me]
    state = jnp.zeros((16, LANES), F32)
    for j in range(count):
        sc.send2[j] = state.astype(BF16)
        if j + 1 < count:
            ending = sc.recv1[j, 0:16].astype(F32)
            total = sc.recv1[j, 32:48].astype(F32)
            state = jnp.exp2(rate * total) * state + ending
    sc.recv2[me] = sc.send2[me]


def backward_starts(count, me, sc):
    rate = sc.lined[me]
    back = jnp.zeros((16, LANES), F32)
    for j in reversed(range(count)):
        sc.send6[j] = back.astype(BF16)
        if j > 0:
            leading = sc.recv1[j, 16:32].astype(F32)
            total = sc.recv1[j, 32:48].astype(F32)
            back = jnp.exp2(rate * total) * back + leading
    sc.recv6[me] = sc.send6[me]


def coefficients(sizes, sc):
    groups, states, steps = sizes
    chunk = lax.broadcasted_iota(jnp.int32, (CHUNKS, LANES), 0)
    zero = jnp.zeros((CHUNKS, LANES), F32)

    def total(value):
        return jnp.sum(value, axis=0, keepdims=True)

    def one(g, carry):
        bias_sum, skip_sum, sig_sum = (zero, zero, zero)
        for i in range(steps):
            skip_sum = skip_sum + sc.items[2, g, i] * sc.items[3, g, i]
            sig_sum = sig_sum + sc.items[1, g, i]
        sc.rows[1, pl.ds(g, 1), :] = total(skip_sum)
        sc.rows[2, pl.ds(g, 1), :] = total(sig_sum)
        before, after = (sc.before[g], sc.after[g])
        for block in range(0, states, SMALL):
            rate, state, back, through, beyond = ([], [], [], [], [])
            for n in range(block, block + SMALL):
                r = jnp.broadcast_to(sc.rate[g, n : n + 1, :], (CHUNKS, LANES))
                rate.append(r)
                state.append(
                    jnp.where(chunk >= 1, shifted_rows(sc.chunk_e[g, n], 1), 0.0)
                )
                back.append(
                    jnp.where(chunk < CHUNKS - 1, shifted_rows(sc.chunk_b[g, n], -1), 0.0)
                )
                through.append(jnp.exp2(r * before))
                beyond.append(jnp.exp2(r * after))

            def ahead(i, carry):
                h, p = carry
                size = sc.items[0, g, i]
                weight = size * sc.items[2, g, i]
                new_h, new_p = ([], [])
                for k in range(SMALL):
                    decay = jnp.exp2(rate[k] * size)
                    moved = decay * h[k]
                    passed = decay * p[k]
                    sc.moved[i, k] = moved
                    sc.passed[i, k] = passed
                    new_h.append(moved + weight * sc.wb[i, block + k])
                    new_p.append(passed)
                return (tuple(new_h), tuple(new_p))

            lax.fori_loop(0, steps, ahead, (tuple(state), tuple(through)), unroll=16)

            def retreat(lap, carry):
                back, beyond, sums = carry
                i = steps - 1 - lap
                size, sig = (sc.items[0, g, i], sc.items[1, g, i])
                scaled = sig * sc.items[2, g, i]
                out = sc.items[3, g, i]
                new_b, new_q, new_s = ([], [], [])
                for k in range(SMALL):
                    grown = rate[k] * size
                    decay = jnp.exp2(grown)
                    moved, passed = (sc.moved[i, k], sc.passed[i, k])
                    write = scaled * sc.wb[i, block + k]
                    adjoint = out * sc.rb[i, block + k] + back[k]
                    steep = adjoint * grown
                    gated = adjoint * sig
                    far = beyond[k] * moved
                    terms = (
                        moved * steep,
                        passed * steep,
                        far * grown,
                        gated * passed,
                        far * sig,
                        beyond[k] * write,
                        adjoint * write,
                        gated * moved,
                    )
                    new_s.append(tuple(a + b for a, b in zip(sums[k], terms)))
                    new_b.append(decay * adjoint)
                    new_q.append(decay * beyond[k])
                return (tuple(new_b), tuple(new_q), tuple(new_s))

            _, _, sums = lax.fori_loop(
                0,
                steps,
                retreat,
                (tuple(back), tuple(beyond), ((zero,) * 8,) * SMALL),
                unroll=8,
            )
            for k in range(SMALL):
                n = block + k
                slope = LN2 * rate[k]
                kept = (
                    sums[k][0],
                    sums[k][1],
                    sums[k][2],
                    slope * sums[k][3],
                    slope * sums[k][4] + sums[k][5],
                )
                for at, value in enumerate(kept):
                    sc.coef[at, n, pl.ds(g, 1), :] = total(value)
                bias_sum = bias_sum + sums[k][6] + slope * sums[k][7]
        sc.rows[0, pl.ds(g, 1), :] = total(bias_sum)
        return carry

    lax.fori_loop(0, groups, one, 0)


def parameter_sums(sizes, sc):
    groups, states, _ = sizes
    sc.starts[:, 0:16] = sc.recv2[...].astype(F32)
    sc.starts[:, 16:32] = sc.recv6[...].astype(F32)
    whole = sc.wide[0, 32:48]
    bias = sc.rows[0]
    for n in range(states):
        state, back = (sc.starts[n, 0:16], sc.starts[n, 16:32])
        rate = sc.lined[n]
        both = state * back * jnp.exp2(rate * whole)
        sc.sums[n] = LN2 * (
            sc.coef[0, n]
            + state * sc.coef[1, n]
            + back * sc.coef[2, n]
            + both * rate * whole
        )
        bias = bias + (
            state * sc.coef[3, n]
            + back * sc.coef[4, n]
            + both * (LN2 * rate) * sc.rows[2]
        )
    for g in range(groups):
        for at, value in ((g, bias[g : g + 1]), (g + groups, sc.rows[1, g : g + 1])):
            row = groups + at % 2
            sc.sums[at // 2, row : row + 1] = value
    sc.send3[...] = sc.sums[...].astype(BF16)


def finish(sizes, y_ref, xg_ref, rg_ref, sc, low, high):
    groups, states, steps = sizes
    chunk = lax.broadcasted_iota(jnp.int32, (CHUNKS, LANES), 0)

    def one(g, carry):
        lanes = pl.ds(pl.multiple_of(g * LANES, LANES), LANES)
        skip = sc.skip[:, lanes]
        before, after = (sc.before[g], sc.after[g])
        for block in range(0, states, BLOCK):
            rate, state, back = ([], [], [])
            for n in range(block, block + BLOCK):
                r = jnp.broadcast_to(sc.rate[g, n : n + 1, :], (CHUNKS, LANES))
                rate.append(r)
                e = jnp.where(chunk >= 1, shifted_rows(sc.chunk_e[g, n], 1), 0.0)
                b = jnp.where(chunk < CHUNKS - 1, shifted_rows(sc.chunk_b[g, n], -1), 0.0)
                state.append(e + jnp.exp2(r * before) * sc.starts[n, pl.ds(g, 1), :])
                back.append(b + jnp.exp2(r * after) * sc.starts[n, pl.ds(16 + g, 1), :])

            def ahead(i, h):
                size = sc.items[0, g, i]
                weight = size * sc.items[2, g, i]
                if block == 0:
                    mixed = skip * sc.items[2, g, i]
                else:
                    mixed = sc.mixed[i]
                new, terms = ([], [])
                for k in range(BLOCK):
                    moved = jnp.exp2(rate[k] * size) * h[k]
                    sc.moved[i, k] = moved
                    value = moved + weight * sc.wb[i, block + k]
                    terms.append(value * sc.rb[i, block + k])
                    new.append(value)
                sc.mixed[i] = mixed + tree(terms)
                return tuple(new)

            lax.fori_loop(0, steps, ahead, tuple(state), unroll=16)

            def retreat(lap, back):
                i = steps - 1 - lap
                size = sc.items[0, g, i]
                out = sc.items[3, g, i]
                new_b, one_w, one_t = ([], [], [])
                for k in range(BLOCK):
                    grown = rate[k] * size
                    adjoint = out * sc.rb[i, block + k] + back[k]
                    one_w.append(adjoint * sc.wb[i, block + k])
                    one_t.append(adjoint * sc.moved[i, k] * rate[k])
                    new_b.append(jnp.exp2(grown) * adjoint)
                written, turned = (tree(one_w), tree(one_t))
                if block > 0:
                    written = written + sc.written[i]
                    turned = turned + sc.turned[i]
                sc.written[i] = written
                sc.turned[i] = turned
                return tuple(new_b)

            lax.fori_loop(0, steps, retreat, tuple(back), unroll=16)
        for i in range(steps):
            size, sig = (sc.items[0, g, i], sc.items[1, g, i])
            x, out = (sc.items[2, g, i], sc.items[3, g, i])
            written = sc.written[i]
            rows = pl.ds(i, CHUNKS, stride=steps)
            sc.nat.at[0][rows, :] = sc.mixed[i]
            sc.nat.at[1][rows, :] = written * size + skip * out
            sc.nat.at[2][rows, :] = (x * written + LN2 * sc.turned[i]) * sig
        y_ref[0, :, lanes] = sc.nat[0].astype(BF16)
        xg_ref[0, :, lanes] = sc.nat[1].astype(BF16)
        rg_ref[0, :, lanes] = sc.nat[2].astype(BF16)
        return carry

    lax.fori_loop(low, high, one, 0)


def window(first, o_ref, dq_ref, sc):
    length, width = sc.q.shape
    scale = 1.0 / math.sqrt(HD)
    docs = sc.doc[...]
    before = jnp.where(first, -1, sc.doc_in[...])
    own = jnp.broadcast_to(docs.astype(F32), (length, length)).T
    own = jnp.concatenate([own, own], axis=1)
    seen = jnp.concatenate([before, docs], axis=1).astype(F32)
    query = lax.broadcasted_iota(jnp.int32, (length, 2 * length), 0)
    key = lax.broadcasted_iota(jnp.int32, (length, 2 * length), 1)
    offset = query + length - key
    allowed = (offset >= 0) & (offset < WINDOW) & (own == seen)
    over_lanes = (((1,), (1,)), ((), ()))
    over_rows = (((0,), (0,)), ((), ()))
    plain = (((1,), (0,)), ((), ()))
    for head in range(width // HD):
        at = slice(head * HD, (head + 1) * HD)
        q, do = (sc.q[:, at], sc.do[:, at])
        k = jnp.concatenate([sc.k_in[:, at], sc.k[:, at]], axis=0)
        v = jnp.concatenate([sc.v_in[:, at], sc.v[:, at]], axis=0)
        scores = lax.dot_general(q, k, over_lanes, preferred_element_type=F32) * scale
        scores = jnp.where(allowed, scores, NEG)
        top = jnp.max(scores, axis=1, keepdims=True)
        raised = jnp.exp(scores - top)
        probs = raised / jnp.sum(raised, axis=1, keepdims=True)
        low = probs.astype(BF16)
        out = lax.dot_general(low, v, plain, preferred_element_type=F32).astype(BF16)
        row_term = jnp.sum(do.astype(F32) * out.astype(F32), axis=1, keepdims=True)
        value_score = lax.dot_general(do, v, over_lanes, preferred_element_type=F32)
        grad = (probs * (value_score - row_term)).astype(BF16)
        o_ref[0, :, at] = out
        dq_ref[0, :, at] = (
            lax.dot_general(grad, k, plain, preferred_element_type=F32) * scale
        ).astype(BF16)
        dk = lax.dot_general(grad, q, over_rows, preferred_element_type=F32) * scale
        dv = lax.dot_general(low, do, over_rows, preferred_element_type=F32)
        sc.dk_out[:, at] = dk[:length].astype(BF16)
        sc.dv_out[:, at] = dv[:length].astype(BF16)
        sc.dk[:, at] = dk[length:]
        sc.dv[:, at] = dv[length:]


def scratch_shapes(sizes, length, width, seq, dp):
    groups, states, steps = sizes
    channels = groups * LANES
    grid = (steps, states, CHUNKS, LANES)
    line = (steps, CHUNKS, LANES)
    return dict(
        x=((length, channels), BF16),
        raw=((length, channels), BF16),
        dy=((length, channels), BF16),
        q=((length, width), BF16),
        k=((length, width), BF16),
        v=((length, width), BF16),
        do=((length, width), BF16),
        bias=((1, channels), F32),
        skip=((1, channels), F32),
        decay=((states, channels), F32),
        write=((1, states, length), BF16),
        read=((1, states, length), BF16),
        doc=((1, length), jnp.int32),
        k_in=((length, width), BF16),
        v_in=((length, width), BF16),
        doc_in=((1, length), jnp.int32),
        dk=((length, width), F32),
        dv=((length, width), F32),
        dk_out=((length, width), BF16),
        dv_out=((length, width), BF16),
        dk_in=((length, width), BF16),
        dv_in=((length, width), BF16),
        rate=((groups, states, LANES), F32),
        lined=((states, 16, LANES), F32),
        coef=((5, states, 16, LANES), F32),
        rows=((3, 16, LANES), F32),
        passed=((steps, SMALL, CHUNKS, LANES), F32),
        wb=(grid, F32),
        rb=(grid, F32),
        nat=((4, length, LANES), F32),
        items=((4, groups) + line, F32),
        before=((groups, CHUNKS, LANES), F32),
        after=((groups, CHUNKS, LANES), F32),
        chunk_e=((groups, states, CHUNKS, LANES), F32),
        chunk_b=((groups, states, CHUNKS, LANES), F32),
        wide=((states, 48, LANES), F32),
        send1=((states, 48, LANES), BF16),
        recv1=((seq, 48, LANES), BF16),
        send2=((seq, 16, LANES), BF16),
        recv2=((states, 16, LANES), BF16),
        send6=((seq, 16, LANES), BF16),
        recv6=((states, 16, LANES), BF16),
        starts=((states, 32, LANES), F32),
        sums=((states, 16, LANES), F32),
        moved=((steps, BLOCK, CHUNKS, LANES), F32),
        mixed=(line, F32),
        written=(line, F32),
        turned=(line, F32),
        send3=((states, 16, LANES), BF16),
        recv3=((seq, 16, LANES), BF16),
        send4=((16, LANES), BF16),
        recv4=((dp, 16, LANES), BF16),
        send5=((16, LANES), BF16),
        recv5=((states, 16, LANES), BF16),
    )


def step_kernel(sizes, seq, dp, names, *refs):
    groups, states, steps = sizes
    hbm = refs[:13]
    y_ref, xg_ref, rg_ref, o_ref, dq_ref, dk_ref, dv_ref = refs[13:20]
    decay_out, skip_out, bias_out = refs[20:23]
    sc = types.SimpleNamespace(**dict(zip(names, refs[23:])))
    load_sem, send_sem, recv_sem, halo_send, halo_recv = refs[23 + len(names) :]
    me = lax.axis_index("seq")
    row = lax.axis_index("dp")
    final = seq - 1

    places = [sc.decay, sc.write, sc.read, sc.bias.at[0], sc.skip.at[0], sc.doc]
    places += [sc.x, sc.raw, sc.dy, sc.q, sc.k, sc.v, sc.do]
    loads = [
        pltpu.make_async_copy(source if at < 6 else source.at[0], place, load_sem.at[at])
        for at, (source, place) in enumerate(zip(hbm, places))
    ]
    for load in loads:
        load.start()
    barrier = pltpu.get_barrier_semaphore()
    for d in range(1, seq):
        pl.semaphore_signal(
            barrier, inc=1, device_id={"seq": lax.rem(me + d, seq)}, device_id_type=MESH
        )
    for d in range(1, dp):
        pl.semaphore_signal(
            barrier, inc=1, device_id={"dp": lax.rem(row + d, dp)}, device_id_type=MESH
        )

    def arrived():
        for load in loads[3:9]:
            load.wait()

    for load in loads[:3]:
        load.wait()
    prepare(sizes, arrived, sc)
    summarize(sizes, sc)
    for load in loads[9:]:
        load.wait()
    pl.semaphore_wait(barrier, seq + dp - 2)

    def stage(at, source, landing, slotted):
        return ("seq", seq, me, source, landing, send_sem.at[at], recv_sem.at[at], slotted)

    def halo(at, source, landing, steps):
        return pltpu.make_async_remote_copy(
            src_ref=source,
            dst_ref=landing,
            send_sem=halo_send.at[at],
            recv_sem=halo_recv.at[at],
            device_id={"seq": lax.rem(me + steps + seq, seq)},
            device_id_type=MESH,
        )

    summed = stage(0, sc.send1, sc.recv1, True)
    copies = exchange(*summed)
    ahead = [halo(0, sc.k, sc.k_in, 1), halo(1, sc.v, sc.v_in, 1), halo(2, sc.doc, sc.doc_in, 1)]
    key_back = halo(3, sc.dk_out, sc.dk_in, -1)
    value_back = halo(4, sc.dv_out, sc.dv_in, -1)

    def attend():
        @pl.when(me > 0)
        def _():
            for copy in ahead:
                copy.wait_recv()

        window(me == 0, o_ref, dq_ref, sc)

    @pl.when(me < final)
    def _():
        for copy in ahead:
            copy.start()
        coefficients(sizes, sc)

    @pl.when(me == 0)
    def _():
        sc.k_in[...] = jnp.zeros(sc.k_in.shape, BF16)
        sc.v_in[...] = jnp.zeros(sc.v_in.shape, BF16)
        sc.doc_in[...] = jnp.zeros(sc.doc_in.shape, jnp.int32)

    @pl.when(me == final)
    def _():
        sc.dk_in[...] = jnp.zeros(sc.dk_in.shape, BF16)
        sc.dv_in[...] = jnp.zeros(sc.dv_in.shape, BF16)

    arrivals(*summed, range(final))
    forward_starts(seq, me, sc)
    forward = stage(1, sc.send2, sc.recv2, True)
    copies += exchange(*forward)
    arrivals(*summed, [final])
    backward_starts(seq, me, sc)
    backward = stage(2, sc.send6, sc.recv6, True)
    copies += exchange(*backward)

    @pl.when(me == final)
    def _():
        coefficients(sizes, sc)

    @pl.when(me < final)
    def _():
        attend()

    arrivals(*forward, range(seq))
    arrivals(*backward, range(seq))
    parameter_sums(sizes, sc)
    reduced = stage(3, sc.send3, sc.recv3, True)
    copies += exchange(*reduced)
    late = lax.div(me, final)
    cut = groups * 2 // 3 * (1 - late)
    middle = groups - late * (groups * 7 // 12)
    finished = functools.partial(finish, sizes, y_ref, xg_ref, rg_ref, sc)

    @pl.when(me == final)
    def _():
        attend()

    finished(0, cut)
    arrivals(*reduced, range(seq))
    sc.recv3[me] = sc.send3[me]
    sc.send4[...] = jnp.sum(sc.recv3[...].astype(F32), axis=0).astype(BF16)
    crossed = ("dp", dp, row, sc.send4, sc.recv4, send_sem.at[4], recv_sem.at[4], False)
    copies += exchange(*crossed)

    @pl.when(me > 0)
    def _():
        key_back.start()

    finished(cut, middle)
    arrivals(*crossed, range(dp))
    sc.recv4[row] = sc.send4[...]
    sc.send5[...] = jnp.sum(sc.recv4[...].astype(F32), axis=0).astype(BF16)
    spread = stage(5, sc.send5, sc.recv5, False)
    copies += exchange(*spread)

    @pl.when(me > 0)
    def _():
        value_back.start()

    finished(middle, groups)

    @pl.when(me < final)
    def _():
        key_back.wait_recv()
        value_back.wait_recv()

    dk_ref[0] = (sc.dk[...] + sc.dk_in[...].astype(F32)).astype(BF16)
    dv_ref[0] = (sc.dv[...] + sc.dv_in[...].astype(F32)).astype(BF16)
    arrivals(*spread, range(seq))
    sc.recv5[me] = sc.send5[...]
    scale = 1.0 / math.sqrt(steps * CHUNKS * seq * dp)
    sc.sums[...] = sc.recv5[...].astype(F32) * scale
    for g in range(groups):
        lanes = slice(g * LANES, (g + 1) * LANES)
        decay_out[:, lanes] = sc.sums[:, g, :]
        bias_out[:, lanes] = sc.sums[g // 2, groups + g % 2 : groups + g % 2 + 1, :]
        h = g + groups
        skip_out[:, lanes] = sc.sums[h // 2, groups + h % 2 : groups + h % 2 + 1, :]
    for copy in copies:
        copy.wait_send()

    @pl.when(me < final)
    def _():
        for copy in ahead:
            copy.wait_send()

    @pl.when(me > 0)
    def _():
        key_back.wait_send()
        value_back.wait_send()


def flush_kernel(*refs):
    count = len(refs) // 2
    sem = refs[-1]
    copies = [
        pltpu.make_async_copy(
            refs[at] if at < count - 2 else refs[at].at[0], refs[count + at], sem.at[at]
        )
        for at in range(count)
    ]
    for copy in copies:
        copy.start()
    for copy in copies:
        copy.wait()


def body(
    mixer_in,
    delta_raw,
    delta_bias,
    decay_log,
    skip_gain,
    state_write,
    state_read,
    mixer_grad,
    attn_query,
    attn_key,
    attn_value,
    attn_grad,
    document_id,
):
    seq, dp = (lax.axis_size("seq"), lax.axis_size("dp"))
    _, length, channels = mixer_in.shape
    width = attn_query.shape[2]
    states = decay_log.shape[1]
    sizes = (channels // LANES, states, length // CHUNKS)
    scratch = scratch_shapes(sizes, length, width, seq, dp)
    inside = pl.BlockSpec(memory_space=pltpu.VMEM)
    outside = pl.BlockSpec(memory_space=pltpu.HBM)
    shapes = (
        [jax.ShapeDtypeStruct(mixer_in.shape, BF16)] * 3
        + [jax.ShapeDtypeStruct(attn_query.shape, BF16)] * 4
        + [jax.ShapeDtypeStruct((states, channels), F32)]
        + [jax.ShapeDtypeStruct((1, channels), F32)] * 2
    )
    operands = (
        decay_log.T,
        state_write.transpose(0, 2, 1),
        state_read.transpose(0, 2, 1),
        delta_bias,
        skip_gain,
        document_id,
        mixer_in,
        delta_raw,
        mixer_grad,
        attn_query,
        attn_key,
        attn_value,
        attn_grad,
    )
    results = pl.pallas_call(
        functools.partial(step_kernel, sizes, seq, dp, tuple(scratch)),
        out_shape=tuple(shapes),
        in_specs=[outside] * 13,
        out_specs=(inside,) * len(shapes),
        scratch_shapes=[pltpu.VMEM(*shape) for shape in scratch.values()]
        + [
            pltpu.SemaphoreType.DMA((13,)),
            pltpu.SemaphoreType.DMA((6, seq)),
            pltpu.SemaphoreType.DMA((6, seq)),
            pltpu.SemaphoreType.DMA((5,)),
            pltpu.SemaphoreType.DMA((5,)),
        ],
        compiler_params=pltpu.CompilerParams(
            collective_id=0, has_side_effects=True, vmem_limit_bytes=48 << 20
        ),
        name="step",
    )(*(pltpu.with_memory_space_constraint(value, pltpu.HBM) for value in operands))
    results = pl.pallas_call(
        flush_kernel,
        out_shape=tuple(shapes[:-2]) + (jax.ShapeDtypeStruct((channels,), F32),) * 2,
        in_specs=[inside] * len(shapes),
        out_specs=(outside,) * len(shapes),
        scratch_shapes=[pltpu.SemaphoreType.DMA((len(shapes),))],
        compiler_params=pltpu.CompilerParams(vmem_limit_bytes=1 << 20),
        name="flush",
    )(*results)
    y, xg, rg, o, dq, dk, dv, decay, skip, bias = results
    return (y, xg, rg, decay.T, skip, bias, o, dq, dk, dv)


def solution(mesh):
    spread = P(("member", "dp"), "seq", "mp")
    shared = P(("member", "dp"), "seq", None)
    one = P(("member", "mp"))
    two = P(("member", "mp"), None)
    return jax.shard_map(
        body,
        mesh=mesh,
        in_specs=(
            spread,
            spread,
            one,
            two,
            one,
            shared,
            shared,
            spread,
            spread,
            spread,
            spread,
            spread,
            P(("member", "dp"), "seq"),
        ),
        out_specs=(spread, spread, spread, two, one, one, spread, spread, spread, spread),
        check_vma=False,
    )
```

```python
import functools
import math
import types

import jax
import jax.numpy as jnp
from jax import lax
from jax.experimental import pallas as pl
from jax.experimental.pallas import tpu as pltpu
from jax.sharding import PartitionSpec as P

HD = 96
WINDOW = 128
CHUNKS = 8
LANES = 128
BLOCK = 8
SMALL = 4
NEG = -1e30
BIG = 1e30
LOG2E = math.log2(math.e)
LN2 = math.log(2.0)
MESH = pl.DeviceIdType.MESH
F32 = jnp.float32
BF16 = jnp.bfloat16


def by_distance(count):
    return sorted(range(1, count), key=lambda d: -min(d, count - d))


def exchange(axis, count, me, source, landing, send_sem, recv_sem, slotted):
    copies = []
    for d in by_distance(count):
        peer = lax.rem(me + d, count)
        copy = pltpu.make_async_remote_copy(
            src_ref=source.at[peer] if slotted else source,
            dst_ref=landing.at[me],
            send_sem=send_sem.at[d],
            recv_sem=recv_sem.at[me],
            device_id={axis: peer},
            device_id_type=MESH,
        )
        copy.start()
        copies.append(copy)
    return copies


def arrivals(axis, count, me, source, landing, send_sem, recv_sem, slotted, origins):
    for j in origins:

        @pl.when(me != j)
        def _():
            pltpu.make_async_remote_copy(
                src_ref=source.at[j] if slotted else source,
                dst_ref=landing.at[j],
                send_sem=send_sem.at[0],
                recv_sem=recv_sem.at[j],
                device_id={axis: j},
                device_id_type=MESH,
            ).wait_recv()


def tree(terms):
    while len(terms) > 1:
        terms = [
            terms[at] + terms[at + 1] if at + 1 < len(terms) else terms[at]
            for at in range(0, len(terms), 2)
        ]
    return terms[0]


def shifted_rows(value, steps):
    return pltpu.roll(value, steps % CHUNKS, 0)


def prepare(sizes, arrived, sc):
    groups, states, steps = sizes
    rate = -LOG2E * jnp.exp(sc.decay[...])
    sc.lined[...] = jnp.zeros(sc.lined.shape, F32)
    for g in range(groups):
        sc.rate[g] = rate[:, g * LANES : (g + 1) * LANES]
        sc.lined[:, g] = rate[:, g * LANES : (g + 1) * LANES]
    for ref in (sc.coef, sc.rows):
        ref[...] = jnp.zeros(ref.shape, F32)
    for source, wide in ((sc.write, sc.wb), (sc.read, sc.rb)):
        sc.nat[0, :, 0:states] = source[0].astype(F32).T
        for i in range(steps):
            rows = sc.nat.at[0][pl.ds(i, CHUNKS, stride=steps), :]
            for n in range(states):
                wide[i, n] = jnp.broadcast_to(rows[:, n : n + 1], (CHUNKS, LANES))
    arrived()

    def one(g, carry):
        lanes = pl.ds(pl.multiple_of(g * LANES, LANES), LANES)
        z = sc.raw[:, lanes].astype(F32) + sc.bias[:, lanes]
        small = jnp.exp(-jnp.abs(z))
        step = jnp.maximum(z, 0.0) + jnp.log(1.0 + small)
        sig = jnp.where(z >= 0, 1.0, small) / (1.0 + small)
        for at, value in enumerate(
            (step, sig, sc.x[:, lanes].astype(F32), sc.dy[:, lanes].astype(F32))
        ):
            sc.nat[at] = value
            for i in range(steps):
                sc.items[at, g, i] = sc.nat.at[at][pl.ds(i, CHUNKS, stride=steps), :]
        return carry

    lax.fori_loop(0, groups, one, 0)


def summarize(sizes, sc):
    groups, states, steps = sizes
    chunk = lax.broadcasted_iota(jnp.int32, (CHUNKS, LANES), 0)

    def one(g, carry):
        total = sc.items[0, g, 0]
        for i in range(1, steps):
            total = total + sc.items[0, g, i]
        ahead, behind = ({1: total}, {1: total})
        for d in (1, 2, 4):
            ahead[2 * d] = ahead[d] + jnp.where(chunk >= d, shifted_rows(ahead[d], d), 0.0)
            behind[2 * d] = behind[d] + jnp.where(
                chunk < CHUNKS - d, shifted_rows(behind[d], -d), 0.0
            )
        sc.before[g] = ahead[8] - total
        sc.after[g] = behind[8] - total
        whole = ahead[8][CHUNKS - 1 : CHUNKS]
        ahead = {d: jnp.where(chunk >= d, ahead[d], BIG) for d in (1, 2, 4)}
        behind = {d: jnp.where(chunk < CHUNKS - d, behind[d], BIG) for d in (1, 2, 4)}

        for block in range(0, states, BLOCK):
            rate = [
                jnp.broadcast_to(sc.rate[g, n : n + 1, :], (CHUNKS, LANES))
                for n in range(block, block + BLOCK)
            ]

            def lap(i, state):
                ending, leading, through = state
                size = sc.items[0, g, i]
                weight = size * sc.items[2, g, i]
                out = sc.items[3, g, i]
                new_e, new_l, new_t = ([], [], [])
                for k in range(BLOCK):
                    decay = jnp.exp2(rate[k] * size)
                    passed = through[k] * decay
                    new_e.append(decay * ending[k] + weight * sc.wb[i, block + k])
                    new_l.append(leading[k] + passed * (out * sc.rb[i, block + k]))
                    new_t.append(passed)
                return (tuple(new_e), tuple(new_l), tuple(new_t))

            zero = jnp.zeros((CHUNKS, LANES), F32)
            ending, leading, _ = lax.fori_loop(
                0,
                steps,
                lap,
                ((zero,) * BLOCK, (zero,) * BLOCK, (jnp.ones((CHUNKS, LANES), F32),) * BLOCK),
                unroll=16,
            )
            for k in range(BLOCK):
                n = block + k
                e, b = (ending[k], leading[k])
                for d in (1, 2, 4):
                    e = e + jnp.exp2(rate[k] * ahead[d]) * shifted_rows(e, d)
                    b = b + jnp.exp2(rate[k] * behind[d]) * shifted_rows(b, -d)
                sc.chunk_e[g, n] = e
                sc.chunk_b[g, n] = b
                sc.wide[n, pl.ds(g, 1), :] = e[CHUNKS - 1 : CHUNKS]
                sc.wide[n, pl.ds(16 + g, 1), :] = b[0:1]
                sc.wide[n, pl.ds(32 + g, 1), :] = whole
        return carry

    sc.wide[...] = jnp.zeros(sc.wide.shape, F32)
    lax.fori_loop(0, groups, one, 0)
    sc.send1[...] = sc.wide[...].astype(BF16)


def forward_starts(count, me, sc):
    sc.recv1[me] = sc.send1[me]
    rate = sc.lined[me]
    state = jnp.zeros((16, LANES), F32)
    for j in range(count):
        sc.send2[j] = state.astype(BF16)
        if j + 1 < count:
            ending = sc.recv1[j, 0:16].astype(F32)
            total = sc.recv1[j, 32:48].astype(F32)
            state = jnp.exp2(rate * total) * state + ending
    sc.recv2[me] = sc.send2[me]


def backward_starts(count, me, sc):
    rate = sc.lined[me]
    back = jnp.zeros((16, LANES), F32)
    for j in reversed(range(count)):
        sc.send6[j] = back.astype(BF16)
        if j > 0:
            leading = sc.recv1[j, 16:32].astype(F32)
            total = sc.recv1[j, 32:48].astype(F32)
            back = jnp.exp2(rate * total) * back + leading
    sc.recv6[me] = sc.send6[me]


def coefficients(sizes, sc, low, high, closing):
    groups, states, steps = sizes
    chunk = lax.broadcasted_iota(jnp.int32, (CHUNKS, LANES), 0)
    zero = jnp.zeros((CHUNKS, LANES), F32)

    def total(value):
        return jnp.sum(value, axis=0, keepdims=True)

    def one(g, carry):
        bias_sum, skip_sum, sig_sum = (zero, zero, zero)
        for i in range(steps):
            skip_sum = skip_sum + sc.items[2, g, i] * sc.items[3, g, i]
            sig_sum = sig_sum + sc.items[1, g, i]
        sc.rows[1, pl.ds(g, 1), :] = total(skip_sum)
        sc.rows[2, pl.ds(g, 1), :] = total(sig_sum)
        before, after = (sc.before[g], sc.after[g])
        for block in range(0, states, SMALL):
            rate, state, back, through, beyond = ([], [], [], [], [])
            for n in range(block, block + SMALL):
                r = jnp.broadcast_to(sc.rate[g, n : n + 1, :], (CHUNKS, LANES))
                rate.append(r)
                state.append(
                    jnp.where(chunk >= 1, shifted_rows(sc.chunk_e[g, n], 1), 0.0)
                )
                back.append(
                    jnp.where(chunk < CHUNKS - 1, shifted_rows(sc.chunk_b[g, n], -1), 0.0)
                )
                through.append(jnp.exp2(r * before))
                beyond.append(jnp.exp2(r * after))

            def ahead(i, carry):
                h, p = carry
                size = sc.items[0, g, i]
                weight = size * sc.items[2, g, i]
                new_h, new_p = ([], [])
                for k in range(SMALL):
                    decay = jnp.exp2(rate[k] * size)
                    moved = decay * h[k]
                    passed = decay * p[k]
                    sc.moved[i, k] = moved
                    sc.passed[i, k] = passed
                    new_h.append(moved + weight * sc.wb[i, block + k])
                    new_p.append(passed)
                return (tuple(new_h), tuple(new_p))

            lax.fori_loop(0, steps, ahead, (tuple(state), tuple(through)), unroll=16)

            def retreat(lap, carry):
                back, beyond, sums = carry
                i = steps - 1 - lap
                size, sig = (sc.items[0, g, i], sc.items[1, g, i])
                scaled = sig * sc.items[2, g, i]
                out = sc.items[3, g, i]
                new_b, new_q, new_s = ([], [], [])
                for k in range(SMALL):
                    grown = rate[k] * size
                    decay = jnp.exp2(grown)
                    moved, passed = (sc.moved[i, k], sc.passed[i, k])
                    write = scaled * sc.wb[i, block + k]
                    adjoint = out * sc.rb[i, block + k] + back[k]
                    steep = adjoint * grown
                    gated = adjoint * sig
                    terms = [
                        moved * steep,
                        passed * steep,
                        gated * passed,
                        adjoint * write,
                        gated * moved,
                    ]
                    if not closing:
                        far = beyond[k] * moved
                        terms += [far * grown, far * sig, beyond[k] * write]
                        new_q.append(decay * beyond[k])
                    new_s.append(tuple(a + b for a, b in zip(sums[k], terms)))
                    new_b.append(decay * adjoint)
                return (tuple(new_b), tuple(new_q), tuple(new_s))

            _, _, sums = lax.fori_loop(
                0,
                steps,
                retreat,
                (
                    tuple(back),
                    () if closing else tuple(beyond),
                    ((zero,) * (5 if closing else 8),) * SMALL,
                ),
                unroll=8,
            )
            for k in range(SMALL):
                n = block + k
                slope = LN2 * rate[k]
                kept = [sums[k][0], sums[k][1], slope * sums[k][2]]
                if not closing:
                    kept += [sums[k][5], slope * sums[k][6] + sums[k][7]]
                for at, value in enumerate(kept):
                    sc.coef[at, n, pl.ds(g, 1), :] = total(value)
                bias_sum = bias_sum + sums[k][3] + slope * sums[k][4]
        sc.rows[0, pl.ds(g, 1), :] = total(bias_sum)
        return carry

    lax.fori_loop(low, high, one, 0)


def parameter_sums(sizes, sc):
    groups, states, _ = sizes
    sc.starts[:, 0:16] = sc.recv2[...].astype(F32)
    sc.starts[:, 16:32] = sc.recv6[...].astype(F32)
    whole = sc.wide[0, 32:48]
    bias = sc.rows[0]
    for n in range(states):
        state, back = (sc.starts[n, 0:16], sc.starts[n, 16:32])
        rate = sc.lined[n]
        both = state * back * jnp.exp2(rate * whole)
        sc.sums[n] = LN2 * (
            sc.coef[0, n]
            + state * sc.coef[1, n]
            + back * sc.coef[3, n]
            + both * rate * whole
        )
        bias = bias + (
            state * sc.coef[2, n]
            + back * sc.coef[4, n]
            + both * (LN2 * rate) * sc.rows[2]
        )
    for g in range(groups):
        for at, value in ((g, bias[g : g + 1]), (g + groups, sc.rows[1, g : g + 1])):
            row = groups + at % 2
            sc.sums[at // 2, row : row + 1] = value
    sc.send3[...] = sc.sums[...].astype(BF16)


def finish(sizes, y_ref, xg_ref, rg_ref, sc, low, high):
    groups, states, steps = sizes
    chunk = lax.broadcasted_iota(jnp.int32, (CHUNKS, LANES), 0)

    def one(g, carry):
        lanes = pl.ds(pl.multiple_of(g * LANES, LANES), LANES)
        skip = sc.skip[:, lanes]
        before, after = (sc.before[g], sc.after[g])
        for block in range(0, states, BLOCK):
            rate, state, back = ([], [], [])
            for n in range(block, block + BLOCK):
                r = jnp.broadcast_to(sc.rate[g, n : n + 1, :], (CHUNKS, LANES))
                rate.append(r)
                e = jnp.where(chunk >= 1, shifted_rows(sc.chunk_e[g, n], 1), 0.0)
                b = jnp.where(chunk < CHUNKS - 1, shifted_rows(sc.chunk_b[g, n], -1), 0.0)
                state.append(e + jnp.exp2(r * before) * sc.starts[n, pl.ds(g, 1), :])
                back.append(b + jnp.exp2(r * after) * sc.starts[n, pl.ds(16 + g, 1), :])

            def ahead(i, h):
                size = sc.items[0, g, i]
                weight = size * sc.items[2, g, i]
                if block == 0:
                    mixed = skip * sc.items[2, g, i]
                else:
                    mixed = sc.mixed[i]
                new, terms = ([], [])
                for k in range(BLOCK):
                    moved = jnp.exp2(rate[k] * size) * h[k]
                    sc.moved[i, k] = moved
                    value = moved + weight * sc.wb[i, block + k]
                    terms.append(value * sc.rb[i, block + k])
                    new.append(value)
                sc.mixed[i] = mixed + tree(terms)
                return tuple(new)

            lax.fori_loop(0, steps, ahead, tuple(state), unroll=16)

            def retreat(lap, back):
                i = steps - 1 - lap
                size = sc.items[0, g, i]
                out = sc.items[3, g, i]
                new_b, one_w, one_t = ([], [], [])
                for k in range(BLOCK):
                    grown = rate[k] * size
                    adjoint = out * sc.rb[i, block + k] + back[k]
                    one_w.append(adjoint * sc.wb[i, block + k])
                    one_t.append(adjoint * sc.moved[i, k] * rate[k])
                    new_b.append(jnp.exp2(grown) * adjoint)
                written, turned = (tree(one_w), tree(one_t))
                if block > 0:
                    written = written + sc.written[i]
                    turned = turned + sc.turned[i]
                sc.written[i] = written
                sc.turned[i] = turned
                return tuple(new_b)

            lax.fori_loop(0, steps, retreat, tuple(back), unroll=16)
        for i in range(steps):
            size, sig = (sc.items[0, g, i], sc.items[1, g, i])
            x, out = (sc.items[2, g, i], sc.items[3, g, i])
            written = sc.written[i]
            rows = pl.ds(i, CHUNKS, stride=steps)
            sc.nat.at[0][rows, :] = sc.mixed[i]
            sc.nat.at[1][rows, :] = written * size + skip * out
            sc.nat.at[2][rows, :] = (x * written + LN2 * sc.turned[i]) * sig
        y_ref[0, :, lanes] = sc.nat[0].astype(BF16)
        xg_ref[0, :, lanes] = sc.nat[1].astype(BF16)
        rg_ref[0, :, lanes] = sc.nat[2].astype(BF16)
        return carry

    lax.fori_loop(low, high, one, 0)


def window(first, o_ref, dq_ref, sc):
    length, width = sc.q.shape
    scale = 1.0 / math.sqrt(HD)
    docs = sc.doc[...]
    before = jnp.where(first, -1, sc.doc_in[...])
    own = jnp.broadcast_to(docs.astype(F32), (length, length)).T
    own = jnp.concatenate([own, own], axis=1)
    seen = jnp.concatenate([before, docs], axis=1).astype(F32)
    query = lax.broadcasted_iota(jnp.int32, (length, 2 * length), 0)
    key = lax.broadcasted_iota(jnp.int32, (length, 2 * length), 1)
    offset = query + length - key
    allowed = (offset >= 0) & (offset < WINDOW) & (own == seen)
    over_lanes = (((1,), (1,)), ((), ()))
    over_rows = (((0,), (0,)), ((), ()))
    plain = (((1,), (0,)), ((), ()))
    for head in range(width // HD):
        at = slice(head * HD, (head + 1) * HD)
        q, do = (sc.q[:, at], sc.do[:, at])
        k = jnp.concatenate([sc.k_in[:, at], sc.k[:, at]], axis=0)
        v = jnp.concatenate([sc.v_in[:, at], sc.v[:, at]], axis=0)
        scores = lax.dot_general(q, k, over_lanes, preferred_element_type=F32) * scale
        scores = jnp.where(allowed, scores, NEG)
        top = jnp.max(scores, axis=1, keepdims=True)
        raised = jnp.exp(scores - top)
        probs = raised / jnp.sum(raised, axis=1, keepdims=True)
        low = probs.astype(BF16)
        out = lax.dot_general(low, v, plain, preferred_element_type=F32).astype(BF16)
        row_term = jnp.sum(do.astype(F32) * out.astype(F32), axis=1, keepdims=True)
        value_score = lax.dot_general(do, v, over_lanes, preferred_element_type=F32)
        grad = (probs * (value_score - row_term)).astype(BF16)
        o_ref[0, :, at] = out
        dq_ref[0, :, at] = (
            lax.dot_general(grad, k, plain, preferred_element_type=F32) * scale
        ).astype(BF16)
        dk = lax.dot_general(grad, q, over_rows, preferred_element_type=F32) * scale
        dv = lax.dot_general(low, do, over_rows, preferred_element_type=F32)
        sc.dk_out[:, at] = dk[:length].astype(BF16)
        sc.dv_out[:, at] = dv[:length].astype(BF16)
        sc.dk[:, at] = dk[length:]
        sc.dv[:, at] = dv[length:]


def scratch_shapes(sizes, length, width, seq, dp):
    groups, states, steps = sizes
    channels = groups * LANES
    grid = (steps, states, CHUNKS, LANES)
    line = (steps, CHUNKS, LANES)
    return dict(
        x=((length, channels), BF16),
        raw=((length, channels), BF16),
        dy=((length, channels), BF16),
        q=((length, width), BF16),
        k=((length, width), BF16),
        v=((length, width), BF16),
        do=((length, width), BF16),
        bias=((1, channels), F32),
        skip=((1, channels), F32),
        decay=((states, channels), F32),
        write=((1, states, length), BF16),
        read=((1, states, length), BF16),
        doc=((1, length), jnp.int32),
        k_in=((length, width), BF16),
        v_in=((length, width), BF16),
        doc_in=((1, length), jnp.int32),
        dk=((length, width), F32),
        dv=((length, width), F32),
        dk_out=((length, width), BF16),
        dv_out=((length, width), BF16),
        dk_in=((length, width), BF16),
        dv_in=((length, width), BF16),
        rate=((groups, states, LANES), F32),
        lined=((states, 16, LANES), F32),
        coef=((5, states, 16, LANES), F32),
        rows=((3, 16, LANES), F32),
        passed=((steps, SMALL, CHUNKS, LANES), F32),
        wb=(grid, F32),
        rb=(grid, F32),
        nat=((4, length, LANES), F32),
        items=((4, groups) + line, F32),
        before=((groups, CHUNKS, LANES), F32),
        after=((groups, CHUNKS, LANES), F32),
        chunk_e=((groups, states, CHUNKS, LANES), F32),
        chunk_b=((groups, states, CHUNKS, LANES), F32),
        wide=((states, 48, LANES), F32),
        send1=((states, 48, LANES), BF16),
        recv1=((seq, 48, LANES), BF16),
        send2=((seq, 16, LANES), BF16),
        recv2=((states, 16, LANES), BF16),
        send6=((seq, 16, LANES), BF16),
        recv6=((states, 16, LANES), BF16),
        starts=((states, 32, LANES), F32),
        sums=((states, 16, LANES), F32),
        moved=((steps, BLOCK, CHUNKS, LANES), F32),
        mixed=(line, F32),
        written=(line, F32),
        turned=(line, F32),
        send3=((states, 16, LANES), BF16),
        recv3=((seq, 16, LANES), BF16),
        send4=((16, LANES), BF16),
        recv4=((dp, 16, LANES), BF16),
        send5=((16, LANES), BF16),
        recv5=((states, 16, LANES), BF16),
    )


def step_kernel(sizes, seq, dp, names, *refs):
    groups, states, steps = sizes
    hbm = refs[:13]
    y_ref, xg_ref, rg_ref, o_ref, dq_ref, dk_ref, dv_ref = refs[13:20]
    decay_out, skip_out, bias_out = refs[20:23]
    sc = types.SimpleNamespace(**dict(zip(names, refs[23:])))
    load_sem, send_sem, recv_sem, halo_send, halo_recv = refs[23 + len(names) :]
    me = lax.axis_index("seq")
    row = lax.axis_index("dp")
    final = seq - 1

    places = [sc.decay, sc.write, sc.read, sc.bias.at[0], sc.skip.at[0], sc.doc]
    places += [sc.x, sc.raw, sc.dy, sc.q, sc.k, sc.v, sc.do]
    loads = [
        pltpu.make_async_copy(source if at < 6 else source.at[0], place, load_sem.at[at])
        for at, (source, place) in enumerate(zip(hbm, places))
    ]
    for load in loads:
        load.start()
    barrier = pltpu.get_barrier_semaphore()
    for d in range(1, seq):
        pl.semaphore_signal(
            barrier, inc=1, device_id={"seq": lax.rem(me + d, seq)}, device_id_type=MESH
        )
    for d in range(1, dp):
        pl.semaphore_signal(
            barrier, inc=1, device_id={"dp": lax.rem(row + d, dp)}, device_id_type=MESH
        )

    def arrived():
        for load in loads[3:9]:
            load.wait()

    for load in loads[:3]:
        load.wait()
    prepare(sizes, arrived, sc)
    summarize(sizes, sc)
    for load in loads[9:]:
        load.wait()
    pl.semaphore_wait(barrier, seq + dp - 2)

    def stage(at, source, landing, slotted):
        return ("seq", seq, me, source, landing, send_sem.at[at], recv_sem.at[at], slotted)

    def halo(at, source, landing, steps):
        return pltpu.make_async_remote_copy(
            src_ref=source,
            dst_ref=landing,
            send_sem=halo_send.at[at],
            recv_sem=halo_recv.at[at],
            device_id={"seq": lax.rem(me + steps + seq, seq)},
            device_id_type=MESH,
        )

    summed = stage(0, sc.send1, sc.recv1, True)
    copies = exchange(*summed)
    ahead = [halo(0, sc.k, sc.k_in, 1), halo(1, sc.v, sc.v_in, 1), halo(2, sc.doc, sc.doc_in, 1)]
    key_back = halo(3, sc.dk_out, sc.dk_in, -1)
    value_back = halo(4, sc.dv_out, sc.dv_in, -1)

    def attend():
        @pl.when(me > 0)
        def _():
            for copy in ahead:
                copy.wait_recv()

        window(me == 0, o_ref, dq_ref, sc)

    late = lax.div(lax.div(4 * me, seq), 3)
    ready = groups - late * (groups * 5 // 12) - lax.div(me, final) * (groups - groups * 5 // 12)

    @pl.when(me < final)
    def _():
        for copy in ahead:
            copy.start()
        coefficients(sizes, sc, 0, ready, False)

    @pl.when(me == 0)
    def _():
        sc.k_in[...] = jnp.zeros(sc.k_in.shape, BF16)
        sc.v_in[...] = jnp.zeros(sc.v_in.shape, BF16)
        sc.doc_in[...] = jnp.zeros(sc.doc_in.shape, jnp.int32)

    @pl.when(me == final)
    def _():
        sc.dk_in[...] = jnp.zeros(sc.dk_in.shape, BF16)
        sc.dv_in[...] = jnp.zeros(sc.dv_in.shape, BF16)

    arrivals(*summed, range(final))
    forward_starts(seq, me, sc)
    forward = stage(1, sc.send2, sc.recv2, True)
    copies += exchange(*forward)
    arrivals(*summed, [final])
    backward_starts(seq, me, sc)
    backward = stage(2, sc.send6, sc.recv6, True)
    copies += exchange(*backward)

    @pl.when(me < final)
    def _():
        coefficients(sizes, sc, ready, groups, False)

    @pl.when(me == final)
    def _():
        coefficients(sizes, sc, 0, groups, True)

    @pl.when(late == 0)
    def _():
        attend()

    arrivals(*forward, range(seq))
    arrivals(*backward, range(seq))
    parameter_sums(sizes, sc)
    reduced = stage(3, sc.send3, sc.recv3, True)
    copies += exchange(*reduced)
    cut = groups * 2 // 3 * (1 - late)
    middle = groups - late * (groups * 7 // 12)
    finished = functools.partial(finish, sizes, y_ref, xg_ref, rg_ref, sc)

    @pl.when(late == 1)
    def _():
        attend()

    finished(0, cut)
    arrivals(*reduced, range(seq))
    sc.recv3[me] = sc.send3[me]
    sc.send4[...] = jnp.sum(sc.recv3[...].astype(F32), axis=0).astype(BF16)
    crossed = ("dp", dp, row, sc.send4, sc.recv4, send_sem.at[4], recv_sem.at[4], False)
    copies += exchange(*crossed)

    @pl.when(me > 0)
    def _():
        key_back.start()

    finished(cut, middle)
    arrivals(*crossed, range(dp))
    sc.recv4[row] = sc.send4[...]
    sc.send5[...] = jnp.sum(sc.recv4[...].astype(F32), axis=0).astype(BF16)
    spread = stage(5, sc.send5, sc.recv5, False)
    copies += exchange(*spread)

    @pl.when(me > 0)
    def _():
        value_back.start()

    finished(middle, groups)

    @pl.when(me < final)
    def _():
        key_back.wait_recv()
        value_back.wait_recv()

    dk_ref[0] = (sc.dk[...] + sc.dk_in[...].astype(F32)).astype(BF16)
    dv_ref[0] = (sc.dv[...] + sc.dv_in[...].astype(F32)).astype(BF16)
    arrivals(*spread, range(seq))
    sc.recv5[me] = sc.send5[...]
    scale = 1.0 / math.sqrt(steps * CHUNKS * seq * dp)
    sc.sums[...] = sc.recv5[...].astype(F32) * scale
    for g in range(groups):
        lanes = slice(g * LANES, (g + 1) * LANES)
        decay_out[:, lanes] = sc.sums[:, g, :]
        bias_out[:, lanes] = sc.sums[g // 2, groups + g % 2 : groups + g % 2 + 1, :]
        h = g + groups
        skip_out[:, lanes] = sc.sums[h // 2, groups + h % 2 : groups + h % 2 + 1, :]
    for copy in copies:
        copy.wait_send()

    @pl.when(me < final)
    def _():
        for copy in ahead:
            copy.wait_send()

    @pl.when(me > 0)
    def _():
        key_back.wait_send()
        value_back.wait_send()


def flush_kernel(*refs):
    count = len(refs) // 2
    sem = refs[-1]
    copies = [
        pltpu.make_async_copy(
            refs[at] if at < count - 2 else refs[at].at[0], refs[count + at], sem.at[at]
        )
        for at in range(count)
    ]
    for copy in copies:
        copy.start()
    for copy in copies:
        copy.wait()


def body(
    mixer_in,
    delta_raw,
    delta_bias,
    decay_log,
    skip_gain,
    state_write,
    state_read,
    mixer_grad,
    attn_query,
    attn_key,
    attn_value,
    attn_grad,
    document_id,
):
    seq, dp = (lax.axis_size("seq"), lax.axis_size("dp"))
    _, length, channels = mixer_in.shape
    width = attn_query.shape[2]
    states = decay_log.shape[1]
    sizes = (channels // LANES, states, length // CHUNKS)
    scratch = scratch_shapes(sizes, length, width, seq, dp)
    inside = pl.BlockSpec(memory_space=pltpu.VMEM)
    outside = pl.BlockSpec(memory_space=pltpu.HBM)
    shapes = (
        [jax.ShapeDtypeStruct(mixer_in.shape, BF16)] * 3
        + [jax.ShapeDtypeStruct(attn_query.shape, BF16)] * 4
        + [jax.ShapeDtypeStruct((states, channels), F32)]
        + [jax.ShapeDtypeStruct((1, channels), F32)] * 2
    )
    operands = (
        decay_log.T,
        state_write.transpose(0, 2, 1),
        state_read.transpose(0, 2, 1),
        delta_bias,
        skip_gain,
        document_id,
        mixer_in,
        delta_raw,
        mixer_grad,
        attn_query,
        attn_key,
        attn_value,
        attn_grad,
    )
    results = pl.pallas_call(
        functools.partial(step_kernel, sizes, seq, dp, tuple(scratch)),
        out_shape=tuple(shapes),
        in_specs=[outside] * 13,
        out_specs=(inside,) * len(shapes),
        scratch_shapes=[pltpu.VMEM(*shape) for shape in scratch.values()]
        + [
            pltpu.SemaphoreType.DMA((13,)),
            pltpu.SemaphoreType.DMA((6, seq)),
            pltpu.SemaphoreType.DMA((6, seq)),
            pltpu.SemaphoreType.DMA((5,)),
            pltpu.SemaphoreType.DMA((5,)),
        ],
        compiler_params=pltpu.CompilerParams(
            collective_id=0, has_side_effects=True, vmem_limit_bytes=48 << 20
        ),
        name="step",
    )(*(pltpu.with_memory_space_constraint(value, pltpu.HBM) for value in operands))
    results = pl.pallas_call(
        flush_kernel,
        out_shape=tuple(shapes[:-2]) + (jax.ShapeDtypeStruct((channels,), F32),) * 2,
        in_specs=[inside] * len(shapes),
        out_specs=(outside,) * len(shapes),
        scratch_shapes=[pltpu.SemaphoreType.DMA((len(shapes),))],
        compiler_params=pltpu.CompilerParams(vmem_limit_bytes=1 << 20),
        name="flush",
    )(*results)
    y, xg, rg, o, dq, dk, dv, decay, skip, bias = results
    return (y, xg, rg, decay.T, skip, bias, o, dq, dk, dv)


def solution(mesh):
    spread = P(("member", "dp"), "seq", "mp")
    shared = P(("member", "dp"), "seq", None)
    one = P(("member", "mp"))
    two = P(("member", "mp"), None)
    return jax.shard_map(
        body,
        mesh=mesh,
        in_specs=(
            spread,
            spread,
            one,
            two,
            one,
            shared,
            shared,
            spread,
            spread,
            spread,
            spread,
            spread,
            P(("member", "dp"), "seq"),
        ),
        out_specs=(spread, spread, spread, two, one, one, spread, spread, spread, spread),
        check_vma=False,
    )
```

```python
import functools
import math
import types

import jax
import jax.numpy as jnp
from jax import lax
from jax.experimental import pallas as pl
from jax.experimental.pallas import tpu as pltpu
from jax.sharding import PartitionSpec as P

HD = 96
WINDOW = 128
CHUNKS = 8
LANES = 128
BLOCK = 8
SMALL = 4
NEG = -1e30
BIG = 1e30
LOG2E = math.log2(math.e)
LN2 = math.log(2.0)
MESH = pl.DeviceIdType.MESH
F32 = jnp.float32
BF16 = jnp.bfloat16


def by_distance(count):
    return sorted(range(1, count), key=lambda d: -min(d, count - d))


def exchange(axis, count, me, source, landing, send_sem, recv_sem, slotted):
    copies = []
    for d in by_distance(count):
        peer = lax.rem(me + d, count)
        copy = pltpu.make_async_remote_copy(
            src_ref=source.at[peer] if slotted else source,
            dst_ref=landing.at[me],
            send_sem=send_sem.at[d],
            recv_sem=recv_sem.at[me],
            device_id={axis: peer},
            device_id_type=MESH,
        )
        copy.start()
        copies.append(copy)
    return copies


def arrivals(axis, count, me, source, landing, send_sem, recv_sem, slotted, origins):
    for j in origins:

        @pl.when(me != j)
        def _():
            pltpu.make_async_remote_copy(
                src_ref=source.at[j] if slotted else source,
                dst_ref=landing.at[j],
                send_sem=send_sem.at[0],
                recv_sem=recv_sem.at[j],
                device_id={axis: j},
                device_id_type=MESH,
            ).wait_recv()


def tree(terms):
    while len(terms) > 1:
        terms = [
            terms[at] + terms[at + 1] if at + 1 < len(terms) else terms[at]
            for at in range(0, len(terms), 2)
        ]
    return terms[0]


def shifted_rows(value, steps):
    return pltpu.roll(value, steps % CHUNKS, 0)


def prepare(sizes, arrived, sc):
    groups, states, steps = sizes
    rate = -LOG2E * jnp.exp(sc.decay[...])
    sc.lined[...] = jnp.zeros(sc.lined.shape, F32)
    for g in range(groups):
        sc.rate[g] = rate[:, g * LANES : (g + 1) * LANES]
        sc.lined[:, g] = rate[:, g * LANES : (g + 1) * LANES]
    for ref in (sc.coef, sc.rows):
        ref[...] = jnp.zeros(ref.shape, F32)
    for source, wide in ((sc.write, sc.wb), (sc.read, sc.rb)):
        sc.nat[0, :, 0:states] = source[0].astype(F32).T
        for i in range(steps):
            rows = sc.nat.at[0][pl.ds(i, CHUNKS, stride=steps), :]
            for n in range(states):
                wide[i, n] = jnp.broadcast_to(rows[:, n : n + 1], (CHUNKS, LANES))
    arrived()

    def one(g, carry):
        lanes = pl.ds(pl.multiple_of(g * LANES, LANES), LANES)
        z = sc.raw[:, lanes].astype(F32) + sc.bias[:, lanes]
        small = jnp.exp(-jnp.abs(z))
        step = jnp.maximum(z, 0.0) + jnp.log(1.0 + small)
        sig = jnp.where(z >= 0, 1.0, small) / (1.0 + small)
        for at, value in enumerate(
            (step, sig, sc.x[:, lanes].astype(F32), sc.dy[:, lanes].astype(F32))
        ):
            sc.nat[at] = value
            for i in range(steps):
                sc.items[at, g, i] = sc.nat.at[at][pl.ds(i, CHUNKS, stride=steps), :]
        return carry

    lax.fori_loop(0, groups, one, 0)


def summarize(sizes, sc):
    groups, states, steps = sizes
    chunk = lax.broadcasted_iota(jnp.int32, (CHUNKS, LANES), 0)

    def one(g, carry):
        total = sc.items[0, g, 0]
        for i in range(1, steps):
            total = total + sc.items[0, g, i]
        ahead, behind = ({1: total}, {1: total})
        for d in (1, 2, 4):
            ahead[2 * d] = ahead[d] + jnp.where(chunk >= d, shifted_rows(ahead[d], d), 0.0)
            behind[2 * d] = behind[d] + jnp.where(
                chunk < CHUNKS - d, shifted_rows(behind[d], -d), 0.0
            )
        sc.before[g] = ahead[8] - total
        sc.after[g] = behind[8] - total
        whole = ahead[8][CHUNKS - 1 : CHUNKS]
        ahead = {d: jnp.where(chunk >= d, ahead[d], BIG) for d in (1, 2, 4)}
        behind = {d: jnp.where(chunk < CHUNKS - d, behind[d], BIG) for d in (1, 2, 4)}

        for block in range(0, states, BLOCK):
            rate = [
                jnp.broadcast_to(sc.rate[g, n : n + 1, :], (CHUNKS, LANES))
                for n in range(block, block + BLOCK)
            ]

            def lap(i, state):
                ending, leading, through = state
                size = sc.items[0, g, i]
                weight = size * sc.items[2, g, i]
                out = sc.items[3, g, i]
                new_e, new_l, new_t = ([], [], [])
                for k in range(BLOCK):
                    decay = jnp.exp2(rate[k] * size)
                    passed = through[k] * decay
                    new_e.append(decay * ending[k] + weight * sc.wb[i, block + k])
                    new_l.append(leading[k] + passed * (out * sc.rb[i, block + k]))
                    new_t.append(passed)
                return (tuple(new_e), tuple(new_l), tuple(new_t))

            zero = jnp.zeros((CHUNKS, LANES), F32)
            ending, leading, _ = lax.fori_loop(
                0,
                steps,
                lap,
                ((zero,) * BLOCK, (zero,) * BLOCK, (jnp.ones((CHUNKS, LANES), F32),) * BLOCK),
                unroll=16,
            )
            for k in range(BLOCK):
                n = block + k
                e, b = (ending[k], leading[k])
                for d in (1, 2, 4):
                    e = e + jnp.exp2(rate[k] * ahead[d]) * shifted_rows(e, d)
                    b = b + jnp.exp2(rate[k] * behind[d]) * shifted_rows(b, -d)
                sc.chunk_e[g, n] = e
                sc.chunk_b[g, n] = b
                sc.wide[n, pl.ds(g, 1), :] = e[CHUNKS - 1 : CHUNKS]
                sc.wide[n, pl.ds(16 + g, 1), :] = b[0:1]
                sc.wide[n, pl.ds(32 + g, 1), :] = whole
        return carry

    sc.wide[...] = jnp.zeros(sc.wide.shape, F32)
    lax.fori_loop(0, groups, one, 0)
    sc.send1[...] = sc.wide[...].astype(BF16)


def forward_starts(count, me, sc):
    sc.recv1[me] = sc.send1[me]
    rate = sc.lined[me]
    state = jnp.zeros((16, LANES), F32)
    for j in range(count):
        sc.send2[j] = state.astype(BF16)
        if j + 1 < count:
            ending = sc.recv1[j, 0:16].astype(F32)
            total = sc.recv1[j, 32:48].astype(F32)
            state = jnp.exp2(rate * total) * state + ending
    sc.recv2[me] = sc.send2[me]


def backward_starts(count, me, sc):
    rate = sc.lined[me]
    back = jnp.zeros((16, LANES), F32)
    for j in reversed(range(count)):
        sc.send6[j] = back.astype(BF16)
        if j > 0:
            leading = sc.recv1[j, 16:32].astype(F32)
            total = sc.recv1[j, 32:48].astype(F32)
            back = jnp.exp2(rate * total) * back + leading
    sc.recv6[me] = sc.send6[me]


def coefficients(sizes, sc, low, high, closing):
    groups, states, steps = sizes
    chunk = lax.broadcasted_iota(jnp.int32, (CHUNKS, LANES), 0)
    zero = jnp.zeros((CHUNKS, LANES), F32)

    def total(value):
        return jnp.sum(value, axis=0, keepdims=True)

    def one(g, carry):
        bias_sum, skip_sum, sig_sum = (zero, zero, zero)
        for i in range(steps):
            skip_sum = skip_sum + sc.items[2, g, i] * sc.items[3, g, i]
            sig_sum = sig_sum + sc.items[1, g, i]
        sc.rows[1, pl.ds(g, 1), :] = total(skip_sum)
        sc.rows[2, pl.ds(g, 1), :] = total(sig_sum)
        before, after = (sc.before[g], sc.after[g])
        for block in range(0, states, SMALL):
            rate, state, back, through, beyond = ([], [], [], [], [])
            for n in range(block, block + SMALL):
                r = jnp.broadcast_to(sc.rate[g, n : n + 1, :], (CHUNKS, LANES))
                rate.append(r)
                state.append(
                    jnp.where(chunk >= 1, shifted_rows(sc.chunk_e[g, n], 1), 0.0)
                )
                back.append(
                    jnp.where(chunk < CHUNKS - 1, shifted_rows(sc.chunk_b[g, n], -1), 0.0)
                )
                through.append(jnp.exp2(r * before))
                beyond.append(jnp.exp2(r * after))

            def ahead(i, carry):
                h, p = carry
                size = sc.items[0, g, i]
                weight = size * sc.items[2, g, i]
                new_h, new_p = ([], [])
                for k in range(SMALL):
                    decay = jnp.exp2(rate[k] * size)
                    moved = decay * h[k]
                    passed = decay * p[k]
                    sc.moved[i, k] = moved
                    sc.passed[i, k] = passed
                    new_h.append(moved + weight * sc.wb[i, block + k])
                    new_p.append(passed)
                return (tuple(new_h), tuple(new_p))

            lax.fori_loop(0, steps, ahead, (tuple(state), tuple(through)), unroll=16)

            def retreat(lap, carry):
                back, beyond, sums = carry
                i = steps - 1 - lap
                size, sig = (sc.items[0, g, i], sc.items[1, g, i])
                scaled = sig * sc.items[2, g, i]
                out = sc.items[3, g, i]
                new_b, new_q, new_s = ([], [], [])
                for k in range(SMALL):
                    grown = rate[k] * size
                    decay = jnp.exp2(grown)
                    moved, passed = (sc.moved[i, k], sc.passed[i, k])
                    write = scaled * sc.wb[i, block + k]
                    adjoint = out * sc.rb[i, block + k] + back[k]
                    steep = adjoint * grown
                    gated = adjoint * sig
                    terms = [
                        moved * steep,
                        passed * steep,
                        gated * passed,
                        adjoint * write,
                        gated * moved,
                    ]
                    if not closing:
                        far = beyond[k] * moved
                        terms += [far * grown, far * sig, beyond[k] * write]
                        new_q.append(decay * beyond[k])
                    new_s.append(tuple(a + b for a, b in zip(sums[k], terms)))
                    new_b.append(decay * adjoint)
                return (tuple(new_b), tuple(new_q), tuple(new_s))

            _, _, sums = lax.fori_loop(
                0,
                steps,
                retreat,
                (
                    tuple(back),
                    () if closing else tuple(beyond),
                    ((zero,) * (5 if closing else 8),) * SMALL,
                ),
                unroll=8,
            )
            for k in range(SMALL):
                n = block + k
                slope = LN2 * rate[k]
                kept = [sums[k][0], sums[k][1], slope * sums[k][2]]
                if not closing:
                    kept += [sums[k][5], slope * sums[k][6] + sums[k][7]]
                for at, value in enumerate(kept):
                    sc.coef[at, n, pl.ds(g, 1), :] = total(value)
                bias_sum = bias_sum + sums[k][3] + slope * sums[k][4]
        sc.rows[0, pl.ds(g, 1), :] = total(bias_sum)
        return carry

    lax.fori_loop(low, high, one, 0)


def parameter_sums(sizes, sc):
    groups, states, _ = sizes
    sc.starts[:, 0:16] = sc.recv2[...].astype(F32)
    sc.starts[:, 16:32] = sc.recv6[...].astype(F32)
    whole = sc.wide[0, 32:48]
    bias = sc.rows[0]
    for n in range(states):
        state, back = (sc.starts[n, 0:16], sc.starts[n, 16:32])
        rate = sc.lined[n]
        both = state * back * jnp.exp2(rate * whole)
        sc.sums[n] = LN2 * (
            sc.coef[0, n]
            + state * sc.coef[1, n]
            + back * sc.coef[3, n]
            + both * rate * whole
        )
        bias = bias + (
            state * sc.coef[2, n]
            + back * sc.coef[4, n]
            + both * (LN2 * rate) * sc.rows[2]
        )
    for g in range(groups):
        for at, value in ((g, bias[g : g + 1]), (g + groups, sc.rows[1, g : g + 1])):
            row = groups + at % 2
            sc.sums[at // 2, row : row + 1] = value
    sc.send3[...] = sc.sums[...].astype(BF16).reshape(sc.send3.shape)


def finish(sizes, y_ref, xg_ref, rg_ref, sc, low, high):
    groups, states, steps = sizes
    chunk = lax.broadcasted_iota(jnp.int32, (CHUNKS, LANES), 0)

    def one(g, carry):
        lanes = pl.ds(pl.multiple_of(g * LANES, LANES), LANES)
        skip = sc.skip[:, lanes]
        before, after = (sc.before[g], sc.after[g])
        for block in range(0, states, BLOCK):
            rate, state, back = ([], [], [])
            for n in range(block, block + BLOCK):
                r = jnp.broadcast_to(sc.rate[g, n : n + 1, :], (CHUNKS, LANES))
                rate.append(r)
                e = jnp.where(chunk >= 1, shifted_rows(sc.chunk_e[g, n], 1), 0.0)
                b = jnp.where(chunk < CHUNKS - 1, shifted_rows(sc.chunk_b[g, n], -1), 0.0)
                state.append(e + jnp.exp2(r * before) * sc.starts[n, pl.ds(g, 1), :])
                back.append(b + jnp.exp2(r * after) * sc.starts[n, pl.ds(16 + g, 1), :])

            def ahead(i, h):
                size = sc.items[0, g, i]
                weight = size * sc.items[2, g, i]
                if block == 0:
                    mixed = skip * sc.items[2, g, i]
                else:
                    mixed = sc.mixed[i]
                new, terms = ([], [])
                for k in range(BLOCK):
                    moved = jnp.exp2(rate[k] * size) * h[k]
                    sc.moved[i, k] = moved
                    value = moved + weight * sc.wb[i, block + k]
                    terms.append(value * sc.rb[i, block + k])
                    new.append(value)
                sc.mixed[i] = mixed + tree(terms)
                return tuple(new)

            lax.fori_loop(0, steps, ahead, tuple(state), unroll=16)

            def retreat(lap, back):
                i = steps - 1 - lap
                size = sc.items[0, g, i]
                out = sc.items[3, g, i]
                new_b, one_w, one_t = ([], [], [])
                for k in range(BLOCK):
                    grown = rate[k] * size
                    adjoint = out * sc.rb[i, block + k] + back[k]
                    one_w.append(adjoint * sc.wb[i, block + k])
                    one_t.append(adjoint * sc.moved[i, k] * rate[k])
                    new_b.append(jnp.exp2(grown) * adjoint)
                written, turned = (tree(one_w), tree(one_t))
                if block > 0:
                    written = written + sc.written[i]
                    turned = turned + sc.turned[i]
                sc.written[i] = written
                sc.turned[i] = turned
                return tuple(new_b)

            lax.fori_loop(0, steps, retreat, tuple(back), unroll=16)
        for i in range(steps):
            size, sig = (sc.items[0, g, i], sc.items[1, g, i])
            x, out = (sc.items[2, g, i], sc.items[3, g, i])
            written = sc.written[i]
            rows = pl.ds(i, CHUNKS, stride=steps)
            sc.nat.at[0][rows, :] = sc.mixed[i]
            sc.nat.at[1][rows, :] = written * size + skip * out
            sc.nat.at[2][rows, :] = (x * written + LN2 * sc.turned[i]) * sig
        y_ref[0, :, lanes] = sc.nat[0].astype(BF16)
        xg_ref[0, :, lanes] = sc.nat[1].astype(BF16)
        rg_ref[0, :, lanes] = sc.nat[2].astype(BF16)
        return carry

    lax.fori_loop(low, high, one, 0)


def window(first, o_ref, dq_ref, sc):
    length, width = sc.q.shape
    scale = 1.0 / math.sqrt(HD)
    docs = sc.doc[...]
    before = jnp.where(first, -1, sc.doc_in[...])
    own = jnp.broadcast_to(docs.astype(F32), (length, length)).T
    own = jnp.concatenate([own, own], axis=1)
    seen = jnp.concatenate([before, docs], axis=1).astype(F32)
    query = lax.broadcasted_iota(jnp.int32, (length, 2 * length), 0)
    key = lax.broadcasted_iota(jnp.int32, (length, 2 * length), 1)
    offset = query + length - key
    allowed = (offset >= 0) & (offset < WINDOW) & (own == seen)
    over_lanes = (((1,), (1,)), ((), ()))
    over_rows = (((0,), (0,)), ((), ()))
    plain = (((1,), (0,)), ((), ()))
    for head in range(width // HD):
        at = slice(head * HD, (head + 1) * HD)
        q, do = (sc.q[:, at], sc.do[:, at])
        k = jnp.concatenate([sc.k_in[:, at], sc.k[:, at]], axis=0)
        v = jnp.concatenate([sc.v_in[:, at], sc.v[:, at]], axis=0)
        scores = lax.dot_general(q, k, over_lanes, preferred_element_type=F32) * scale
        scores = jnp.where(allowed, scores, NEG)
        top = jnp.max(scores, axis=1, keepdims=True)
        raised = jnp.exp(scores - top)
        probs = raised / jnp.sum(raised, axis=1, keepdims=True)
        low = probs.astype(BF16)
        out = lax.dot_general(low, v, plain, preferred_element_type=F32).astype(BF16)
        row_term = jnp.sum(do.astype(F32) * out.astype(F32), axis=1, keepdims=True)
        value_score = lax.dot_general(do, v, over_lanes, preferred_element_type=F32)
        grad = (probs * (value_score - row_term)).astype(BF16)
        o_ref[0, :, at] = out
        dq_ref[0, :, at] = (
            lax.dot_general(grad, k, plain, preferred_element_type=F32) * scale
        ).astype(BF16)
        dk = lax.dot_general(grad, q, over_rows, preferred_element_type=F32) * scale
        dv = lax.dot_general(low, do, over_rows, preferred_element_type=F32)
        sc.dk_out[:, at] = dk[:length].astype(BF16)
        sc.dv_out[:, at] = dv[:length].astype(BF16)
        sc.dk[:, at] = dk[length:]
        sc.dv[:, at] = dv[length:]


def scratch_shapes(sizes, length, width, seq, dp):
    groups, states, steps = sizes
    channels = groups * LANES
    grid = (steps, states, CHUNKS, LANES)
    line = (steps, CHUNKS, LANES)
    return dict(
        x=((length, channels), BF16),
        raw=((length, channels), BF16),
        dy=((length, channels), BF16),
        q=((length, width), BF16),
        k=((length, width), BF16),
        v=((length, width), BF16),
        do=((length, width), BF16),
        bias=((1, channels), F32),
        skip=((1, channels), F32),
        decay=((states, channels), F32),
        write=((1, states, length), BF16),
        read=((1, states, length), BF16),
        doc=((1, length), jnp.int32),
        k_in=((length, width), BF16),
        v_in=((length, width), BF16),
        doc_in=((1, length), jnp.int32),
        dk=((length, width), F32),
        dv=((length, width), F32),
        dk_out=((length, width), BF16),
        dv_out=((length, width), BF16),
        dk_in=((length, width), BF16),
        dv_in=((length, width), BF16),
        rate=((groups, states, LANES), F32),
        lined=((states, 16, LANES), F32),
        coef=((5, states, 16, LANES), F32),
        rows=((3, 16, LANES), F32),
        passed=((steps, SMALL, CHUNKS, LANES), F32),
        wb=(grid, F32),
        rb=(grid, F32),
        nat=((4, length, LANES), F32),
        items=((4, groups) + line, F32),
        before=((groups, CHUNKS, LANES), F32),
        after=((groups, CHUNKS, LANES), F32),
        chunk_e=((groups, states, CHUNKS, LANES), F32),
        chunk_b=((groups, states, CHUNKS, LANES), F32),
        wide=((states, 48, LANES), F32),
        send1=((states, 48, LANES), BF16),
        recv1=((seq, 48, LANES), BF16),
        send2=((seq, 16, LANES), BF16),
        recv2=((states, 16, LANES), BF16),
        send6=((seq, 16, LANES), BF16),
        recv6=((states, 16, LANES), BF16),
        starts=((states, 32, LANES), F32),
        sums=((states, 16, LANES), F32),
        moved=((steps, BLOCK, CHUNKS, LANES), F32),
        mixed=(line, F32),
        written=(line, F32),
        turned=(line, F32),
        send3=((dp, states // dp, 16, LANES), BF16),
        recv3=((dp, states // dp, 16, LANES), BF16),
        send4=((states // dp, 16, LANES), BF16),
        recv4=((seq, states // dp, 16, LANES), BF16),
        send5=((states // dp, 16, LANES), BF16),
        recv5=((dp, states // dp, 16, LANES), BF16),
    )


def step_kernel(sizes, seq, dp, names, *refs):
    groups, states, steps = sizes
    hbm = refs[:13]
    y_ref, xg_ref, rg_ref, o_ref, dq_ref, dk_ref, dv_ref = refs[13:20]
    decay_out, skip_out, bias_out = refs[20:23]
    sc = types.SimpleNamespace(**dict(zip(names, refs[23:])))
    load_sem, send_sem, recv_sem, halo_send, halo_recv = refs[23 + len(names) :]
    me = lax.axis_index("seq")
    row = lax.axis_index("dp")
    final = seq - 1

    places = [sc.decay, sc.write, sc.read, sc.bias.at[0], sc.skip.at[0], sc.doc]
    places += [sc.x, sc.raw, sc.dy, sc.q, sc.k, sc.v, sc.do]
    loads = [
        pltpu.make_async_copy(source if at < 6 else source.at[0], place, load_sem.at[at])
        for at, (source, place) in enumerate(zip(hbm, places))
    ]
    for load in loads:
        load.start()
    barrier = pltpu.get_barrier_semaphore()
    for d in range(1, seq):
        pl.semaphore_signal(
            barrier, inc=1, device_id={"seq": lax.rem(me + d, seq)}, device_id_type=MESH
        )
    for d in range(1, dp):
        pl.semaphore_signal(
            barrier, inc=1, device_id={"dp": lax.rem(row + d, dp)}, device_id_type=MESH
        )

    def arrived():
        for load in loads[3:9]:
            load.wait()

    for load in loads[:3]:
        load.wait()
    prepare(sizes, arrived, sc)
    summarize(sizes, sc)
    for load in loads[9:]:
        load.wait()
    pl.semaphore_wait(barrier, seq + dp - 2)

    def stage(at, source, landing, slotted):
        return ("seq", seq, me, source, landing, send_sem.at[at], recv_sem.at[at], slotted)

    def halo(at, source, landing, steps):
        return pltpu.make_async_remote_copy(
            src_ref=source,
            dst_ref=landing,
            send_sem=halo_send.at[at],
            recv_sem=halo_recv.at[at],
            device_id={"seq": lax.rem(me + steps + seq, seq)},
            device_id_type=MESH,
        )

    summed = stage(0, sc.send1, sc.recv1, True)
    copies = exchange(*summed)
    ahead = [halo(0, sc.k, sc.k_in, 1), halo(1, sc.v, sc.v_in, 1), halo(2, sc.doc, sc.doc_in, 1)]
    key_back = halo(3, sc.dk_out, sc.dk_in, -1)
    value_back = halo(4, sc.dv_out, sc.dv_in, -1)

    def attend():
        @pl.when(me > 0)
        def _():
            for copy in ahead:
                copy.wait_recv()

        window(me == 0, o_ref, dq_ref, sc)

    late = lax.div(lax.div(4 * me, seq), 3)
    ready = groups - late * (groups * 5 // 12) - lax.div(me, final) * (groups - groups * 5 // 12)

    @pl.when(me < final)
    def _():
        for copy in ahead:
            copy.start()
        coefficients(sizes, sc, 0, ready, False)

    @pl.when(me == 0)
    def _():
        sc.k_in[...] = jnp.zeros(sc.k_in.shape, BF16)
        sc.v_in[...] = jnp.zeros(sc.v_in.shape, BF16)
        sc.doc_in[...] = jnp.zeros(sc.doc_in.shape, jnp.int32)

    @pl.when(me == final)
    def _():
        sc.dk_in[...] = jnp.zeros(sc.dk_in.shape, BF16)
        sc.dv_in[...] = jnp.zeros(sc.dv_in.shape, BF16)

    arrivals(*summed, range(final))
    forward_starts(seq, me, sc)
    forward = stage(1, sc.send2, sc.recv2, True)
    copies += exchange(*forward)
    arrivals(*summed, [final])
    backward_starts(seq, me, sc)
    backward = stage(2, sc.send6, sc.recv6, True)
    copies += exchange(*backward)

    @pl.when(me < final)
    def _():
        coefficients(sizes, sc, ready, groups, False)

    @pl.when(me == final)
    def _():
        coefficients(sizes, sc, 0, groups, True)

    @pl.when(late == 0)
    def _():
        attend()

    arrivals(*forward, range(seq))
    arrivals(*backward, range(seq))
    parameter_sums(sizes, sc)
    def across(at, source, landing, slotted):
        return ("dp", dp, row, source, landing, send_sem.at[at], recv_sem.at[at], slotted)

    reduced = across(3, sc.send3, sc.recv3, True)
    copies += exchange(*reduced)
    cut = groups * 5 // 12 * (1 - late)
    middle = groups - late * (groups // 3)
    finished = functools.partial(finish, sizes, y_ref, xg_ref, rg_ref, sc)

    @pl.when(me * (1 - late) > 0)
    def _():
        key_back.start()

    @pl.when(late == 1)
    def _():
        attend()

    finished(0, cut)
    arrivals(*reduced, range(dp))
    sc.recv3[row] = sc.send3[row]
    sc.send4[...] = jnp.sum(sc.recv3[...].astype(F32), axis=0).astype(BF16)
    crossed = stage(4, sc.send4, sc.recv4, False)
    copies += exchange(*crossed)

    @pl.when(late == 1)
    def _():
        key_back.start()

    finished(cut, middle)
    arrivals(*crossed, range(seq))
    sc.recv4[me] = sc.send4[...]
    sc.send5[...] = jnp.sum(sc.recv4[...].astype(F32), axis=0).astype(BF16)
    spread = across(5, sc.send5, sc.recv5, False)
    copies += exchange(*spread)

    @pl.when(me > 0)
    def _():
        value_back.start()

    finished(middle, groups)

    @pl.when(me < final)
    def _():
        key_back.wait_recv()
        value_back.wait_recv()

    dk_ref[0] = (sc.dk[...] + sc.dk_in[...].astype(F32)).astype(BF16)
    dv_ref[0] = (sc.dv[...] + sc.dv_in[...].astype(F32)).astype(BF16)
    arrivals(*spread, range(dp))
    sc.recv5[row] = sc.send5[...]
    scale = 1.0 / math.sqrt(steps * CHUNKS * seq * dp)
    sc.sums[...] = sc.recv5[...].astype(F32).reshape(sc.sums.shape) * scale
    for g in range(groups):
        lanes = slice(g * LANES, (g + 1) * LANES)
        decay_out[:, lanes] = sc.sums[:, g, :]
        bias_out[:, lanes] = sc.sums[g // 2, groups + g % 2 : groups + g % 2 + 1, :]
        h = g + groups
        skip_out[:, lanes] = sc.sums[h // 2, groups + h % 2 : groups + h % 2 + 1, :]
    for copy in copies:
        copy.wait_send()

    @pl.when(me < final)
    def _():
        for copy in ahead:
            copy.wait_send()

    @pl.when(me > 0)
    def _():
        key_back.wait_send()
        value_back.wait_send()


def flush_kernel(*refs):
    count = len(refs) // 2
    sem = refs[-1]
    copies = [
        pltpu.make_async_copy(
            refs[at] if at < count - 2 else refs[at].at[0], refs[count + at], sem.at[at]
        )
        for at in range(count)
    ]
    for copy in copies:
        copy.start()
    for copy in copies:
        copy.wait()


def body(
    mixer_in,
    delta_raw,
    delta_bias,
    decay_log,
    skip_gain,
    state_write,
    state_read,
    mixer_grad,
    attn_query,
    attn_key,
    attn_value,
    attn_grad,
    document_id,
):
    seq, dp = (lax.axis_size("seq"), lax.axis_size("dp"))
    _, length, channels = mixer_in.shape
    width = attn_query.shape[2]
    states = decay_log.shape[1]
    sizes = (channels // LANES, states, length // CHUNKS)
    scratch = scratch_shapes(sizes, length, width, seq, dp)
    inside = pl.BlockSpec(memory_space=pltpu.VMEM)
    outside = pl.BlockSpec(memory_space=pltpu.HBM)
    shapes = (
        [jax.ShapeDtypeStruct(mixer_in.shape, BF16)] * 3
        + [jax.ShapeDtypeStruct(attn_query.shape, BF16)] * 4
        + [jax.ShapeDtypeStruct((states, channels), F32)]
        + [jax.ShapeDtypeStruct((1, channels), F32)] * 2
    )
    operands = (
        decay_log.T,
        state_write.transpose(0, 2, 1),
        state_read.transpose(0, 2, 1),
        delta_bias,
        skip_gain,
        document_id,
        mixer_in,
        delta_raw,
        mixer_grad,
        attn_query,
        attn_key,
        attn_value,
        attn_grad,
    )
    results = pl.pallas_call(
        functools.partial(step_kernel, sizes, seq, dp, tuple(scratch)),
        out_shape=tuple(shapes),
        in_specs=[outside] * 13,
        out_specs=(inside,) * len(shapes),
        scratch_shapes=[pltpu.VMEM(*shape) for shape in scratch.values()]
        + [
            pltpu.SemaphoreType.DMA((13,)),
            pltpu.SemaphoreType.DMA((6, seq)),
            pltpu.SemaphoreType.DMA((6, seq)),
            pltpu.SemaphoreType.DMA((5,)),
            pltpu.SemaphoreType.DMA((5,)),
        ],
        compiler_params=pltpu.CompilerParams(
            collective_id=0, has_side_effects=True, vmem_limit_bytes=48 << 20
        ),
        name="step",
    )(*(pltpu.with_memory_space_constraint(value, pltpu.HBM) for value in operands))
    results = pl.pallas_call(
        flush_kernel,
        out_shape=tuple(shapes[:-2]) + (jax.ShapeDtypeStruct((channels,), F32),) * 2,
        in_specs=[inside] * len(shapes),
        out_specs=(outside,) * len(shapes),
        scratch_shapes=[pltpu.SemaphoreType.DMA((len(shapes),))],
        compiler_params=pltpu.CompilerParams(vmem_limit_bytes=1 << 20),
        name="flush",
    )(*results)
    y, xg, rg, o, dq, dk, dv, decay, skip, bias = results
    return (y, xg, rg, decay.T, skip, bias, o, dq, dk, dv)


def solution(mesh):
    spread = P(("member", "dp"), "seq", "mp")
    shared = P(("member", "dp"), "seq", None)
    one = P(("member", "mp"))
    two = P(("member", "mp"), None)
    return jax.shard_map(
        body,
        mesh=mesh,
        in_specs=(
            spread,
            spread,
            one,
            two,
            one,
            shared,
            shared,
            spread,
            spread,
            spread,
            spread,
            spread,
            P(("member", "dp"), "seq"),
        ),
        out_specs=(spread, spread, spread, two, one, one, spread, spread, spread, spread),
        check_vma=False,
    )
```
